256 devices in a mesh: dp: 32 (over x, y, core), expert: 8 (over z).
Axes of the slice: x: 4, y: 4, z: 8, core: 2. Of those that a mesh axis runs over, the one named last changes fastest.
Arguments:
- tokens: bfloat16 [1024, 4096], P('expert', 'dp'), may hold values from -6 to 6
- in_signs: int32 [1024, 128], P('expert', 'dp'), may hold values from -2147483648 to 2147483646
- out_signs: int32 [1024, 224], P('expert'), may hold values from -2147483648 to 2147483646
- expert_ids: int32 [1024, 2], P('expert'), may hold values from 0 to 7, all different within a row; in each aligned block of 128 rows (0 to 127, 128 to 255, ...) at most 40 rows name the same one
- route_weight: float32 [1024, 2], P('expert'), may hold values from 0.2 to 1
- cotangent: bfloat16 [1024, 7168], P('expert', 'dp'), may hold values from -6 to 6
- mean_weight: bfloat16 [8, 4096, 7168], P('expert', 'dp'), may hold values from -0.09375 to 0.09375
- rho_weight: bfloat16 [8, 4096, 7168], P('expert', 'dp'), may hold values from -6 to -3
- noise_weight: bfloat16 [8, 4096, 7168], P('expert', 'dp'), may hold values from -4 to 4
Outputs:
- hidden_out: bfloat16 [1024, 7168], P('expert', 'dp')
- grad_tokens: bfloat16 [1024, 4096], P('expert', 'dp')
- grad_mean: bfloat16 [8, 4096, 7168], P('expert', 'dp')
- grad_rho: bfloat16 [8, 4096, 7168], P('expert', 'dp')
The draws below stay inside these ranges and needn't reach their ends.
Inputs may be any that keep to these rules, and one draw needn't show every extreme that they name: `expert_ids`: each token names 2 different experts. In each aligned block of 128 tokens no expert is named by more than 40 tokens, and in some blocks one expert is named by exactly 40. `in_signs`: bit b of word w, counted from the lowest, is set where the sign of feature 32 * w + b is -1 and clear where it is +1. `out_signs`: bit b of word w, counted from the lowest, is set where the sign of hidden unit 32 * w + b is -1 and clear where it is +1.
All inputs are finite; a program needn't handle non-finite values.
Results may differ from the reference program's by a relative error of at most 0.0071.
Values may be sent and summed in bfloat16 or wider, within the bound.
No kernel may reach another device: no remote copies, remote signals or barrier semaphores. Data moves between devices by JAX's collectives and lax.ppermute only.
A program may use at most 128 MiB of HBM per device.

```python
import math
import jax
import jax.numpy as jnp
import numpy as np
from jax import lax

D = 4096
FF = 7168
TOPK = 2
TOK_DEV = 128
EXPERTS = 8
CAP = 40
TOKENS = 1024
N_EXPERT = 8


def with_ends(array, stream_key, low, top_value):
    shape = array.shape
    index_at = [jax.random.randint(jax.random.fold_in(stream_key, axis), (), 0, shape[axis]) for axis in range(len(shape))]
    array = array.at[tuple(index_at)].set(low)
    longest = shape.index(max(shape))
    index_at[longest] = (index_at[longest] + 1) % shape[longest]
    return array.at[tuple(index_at)].set(top_value)


def block_scale(rng, extent, pieces, least, high):
    def one(axis_at, blocks):
        steps = jax.random.uniform(jax.random.fold_in(jax.random.fold_in(rng, 6), axis_at), (blocks,), jnp.float32, least / len(pieces), high / len(pieces))
        return jnp.repeat(jnp.exp(steps), extent[axis_at] // blocks).reshape((-1,) + (1,) * (len(extent) - axis_at - 1))

    loudness = one(*pieces[0])
    for cut in pieces[1:]:
        loudness = loudness * one(*cut)
    return loudness


def shared_out(key, own, number, rows, number_of, top, limit, skew):
    ranking = jax.random.permutation(key, number_of)
    heavy_load, common = shares(number_of, rows * top, limit, skew, True), shares(number_of, rows * top, limit, skew, False)
    places = jnp.arange(number_of)

    def named(sizes, turn):
        used = int((sizes > 0).sum())
        fixed = max(1, used // 4)
        moved = fixed + (places - fixed + turn * (used - fixed)) % max(1, number_of - fixed)
        return jnp.zeros((number_of,), jnp.int32).at[ranking[jnp.where(places < fixed, places, moved)]].set(jnp.asarray(sizes, jnp.int32))

    sizes = jnp.where(number % 4 == 0, named(heavy_load, number // 4), named(common, number - number // 4 - 1))
    mixed = jax.random.permutation(jax.random.fold_in(own, 3), number_of)
    giver, sink = mixed[0:number_of // 2 * 2:2], mixed[1:number_of // 2 * 2:2]
    slack = jnp.minimum(sizes[giver] - 1, limit - sizes[sink]) // 2
    slack = jnp.where((giver == ranking[0]) | (sink == ranking[0]) | (sizes[sink] == 0), 0, jnp.maximum(slack, 0))
    moved = jax.random.randint(jax.random.fold_in(own, 4), (number_of // 2,), 0, 1 << 20) % (slack + 1)
    sizes = sizes.at[giver].add(-moved).at[sink].add(moved)
    members = jnp.searchsorted(jnp.cumsum(sizes), jnp.arange(rows * top), side="right").astype(jnp.int32)
    listing = members.reshape(top, rows).T
    listing = listing[jax.random.permutation(jax.random.fold_in(own, 1), rows)]
    turn = jax.random.randint(jax.random.fold_in(own, 2), (rows, 1), 0, top)
    return jnp.take_along_axis(listing, (jnp.arange(top)[None, :] + turn) % top, axis=1)


def shares(count, total, limit, skew, full):
    weights = [(1 << 20) // math.isqrt(grade ** skew) + 1 for grade in range(1, count + 1)]
    largest = limit if full else min(limit, max(-(-total // count), total * weights[0] // sum(weights)))
    least = 1 if total - largest >= count - 1 else 0
    holding, surplus = [largest] + [least] * (count - 1), total - largest - least * (count - 1)
    while surplus > 0:
        free = [i for i in range(1, count) if holding[i] < largest] or [i for i in range(1, count) if holding[i] < limit]
        whole, remaining = sum([weights[i] for i in free]), surplus
        for i in free:
            more = min(limit - holding[i], max(1, remaining * weights[i] // whole), surplus)
            holding[i] = holding[i] + more
            surplus = surplus - more
    return np.array(holding)


def bell_draw(key, dims, deviation, most, cuts=(), kind=jnp.bfloat16):
    entries = jax.random.normal(key, dims, jnp.float32) * deviation
    if len(cuts) > 0:
        entries = block_scale(key, dims, cuts, -0.22, 0.18) * entries
    return jnp.clip(entries, min=-most, max=most).astype(kind)


def setup_inputs(seed: int = 0) -> dict:
    key_list = jax.random.split(jax.random.key(seed), 10)
    tokens = bell_draw(key_list[0], (TOKENS, D), 1.0, 6.0, ((0, 8), (1, 32)))
    in_signs = with_ends(jax.random.randint(key_list[1], (TOKENS, D // 32), -2147483648, 2147483647), jax.random.fold_in(key_list[1], 1), -2147483648, 2147483646).astype(jnp.int32)
    out_signs = with_ends(jax.random.randint(key_list[2], (TOKENS, FF // 32), -2147483648, 2147483647), jax.random.fold_in(key_list[2], 1), -2147483648, 2147483646).astype(jnp.int32)
    expert_ids_keys = jax.random.split(jax.random.fold_in(key_list[3], 1), TOKENS // TOK_DEV)
    expert_ids_turns = jax.random.permutation(jax.random.fold_in(key_list[3], 3), TOKENS // TOK_DEV)
    expert_ids = jax.vmap(lambda own, number: shared_out(jax.random.fold_in(key_list[3], 2), own, number, TOK_DEV, EXPERTS, TOPK, CAP, 2))(expert_ids_keys, expert_ids_turns).reshape((TOKENS, TOPK))
    route_weight = jnp.clip(0.2 + 0.8 * jax.random.uniform(key_list[4], (TOKENS, TOPK), jnp.float32) ** block_scale(key_list[4], (TOKENS, TOPK), ((0, 8),), -0.2, 0.2), 0.2, 1.0)
    cotangent = bell_draw(key_list[5], (TOKENS, FF), 1.0, 6.0, ((0, 8), (1, 32)))
    mean_weight = bell_draw(key_list[6], (EXPERTS, D, FF), D ** -0.5, 0.09375, ((0, 8), (1, 32)))
    rho_weight = jnp.clip(-6.0 + 3.0 * jax.random.uniform(key_list[7], (EXPERTS, D, FF), jnp.float32) ** block_scale(key_list[7], (EXPERTS, D, FF), ((0, 8), (1, 32)), -0.2, 0.2), -6.0, -3.0).astype(jnp.bfloat16)
    noise_weight = bell_draw(key_list[8], (EXPERTS, D, FF), 1.0, 4.0, ((0, 8), (1, 32)))
    return dict(tokens=tokens, in_signs=in_signs, out_signs=out_signs, expert_ids=expert_ids, route_weight=route_weight, cotangent=cotangent, mean_weight=mean_weight, rho_weight=rho_weight, noise_weight=noise_weight)


def unpack_rows(words):
    shifts = jnp.arange(32, dtype=jnp.int32)
    bits = jnp.bitwise_and(jnp.right_shift(words[..., None], shifts), 1)
    signs = (1 - 2 * bits).astype(jnp.float32)
    return signs.reshape(words.shape[:-1] + (words.shape[-1] * 32,))


def block_slots(block_ids):
    onehot = (block_ids[:, :, None] == jnp.arange(EXPERTS, dtype=jnp.int32)).astype(jnp.int32)
    flat = onehot.reshape(-1, EXPERTS)
    before = (jnp.cumsum(flat, axis=0) - flat).astype(jnp.int32)
    return jnp.sum(before * flat, axis=1).astype(jnp.int32).reshape(block_ids.shape)


def reference(tokens, in_signs, out_signs, expert_ids, route_weight, cotangent, mean_weight, rho_weight, noise_weight):
    blocks = expert_ids.reshape(N_EXPERT, TOK_DEV, TOPK)
    ranks = jax.vmap(block_slots)(blocks)
    source = jnp.arange(N_EXPERT, dtype=jnp.int32)[:, None, None]
    per_expert = N_EXPERT * CAP
    position = (blocks * per_expert + source * CAP + ranks).astype(jnp.int32).reshape(TOKENS, TOPK)
    total = EXPERTS * per_expert
    token_index = jnp.broadcast_to(jnp.arange(TOKENS, dtype=jnp.int32)[:, None], (TOKENS, TOPK))
    flat_pos = position.reshape(-1)
    slot_token = jnp.zeros((total,), jnp.int32).at[flat_pos].set(token_index.reshape(-1))
    slot_fill = jnp.zeros((total,), jnp.float32).at[flat_pos].set(1.0)
    slot_weight = jnp.zeros((total,), jnp.float32).at[flat_pos].set(route_weight.reshape(-1))
    input_full = unpack_rows(in_signs)
    output_full = unpack_rows(out_signs)

    def one_expert(operands):
        mean_e, rho_e, noise_e, tok_e, fill_e, weight_e = operands
        rows = jnp.take(tokens, tok_e, axis=0) * fill_e[:, None].astype(jnp.bfloat16)
        input_rows = jnp.take(input_full, tok_e, axis=0)
        output_rows = jnp.take(output_full, tok_e, axis=0)
        signed = rows * input_rows.astype(jnp.bfloat16)
        rho_float = rho_e.astype(jnp.float32)
        noise_float = noise_e.astype(jnp.float32)
        delta = (jax.nn.softplus(rho_float) * noise_float).astype(jnp.bfloat16)
        mean_part = jnp.dot(rows, mean_e, preferred_element_type=jnp.float32)
        pert_part = jnp.dot(signed, delta, preferred_element_type=jnp.float32)
        preact = mean_part + output_rows * pert_part
        gate = jax.nn.sigmoid(preact)
        hidden = (preact * gate).astype(jnp.bfloat16)
        upstream = (jnp.take(cotangent, tok_e, axis=0).astype(jnp.float32) * weight_e[:, None]).astype(jnp.bfloat16)
        slope = gate * (1.0 + preact * (1.0 - gate))
        grad_preact = (upstream.astype(jnp.float32) * slope).astype(jnp.bfloat16)
        grad_signed_pre = grad_preact * output_rows.astype(jnp.bfloat16)
        grad_mean_e = jnp.dot(rows.T, grad_preact, preferred_element_type=jnp.float32).astype(jnp.bfloat16)
        grad_delta = jnp.dot(signed.T, grad_signed_pre, preferred_element_type=jnp.float32)
        grad_rho_e = (grad_delta * noise_float * jax.nn.sigmoid(rho_float)).astype(jnp.bfloat16)
        back = jnp.dot(grad_preact, mean_e.T, preferred_element_type=jnp.float32)
        back = back + input_rows * jnp.dot(grad_signed_pre, delta.T, preferred_element_type=jnp.float32)
        return hidden, back.astype(jnp.bfloat16), grad_mean_e, grad_rho_e

    operands = (mean_weight, rho_weight, noise_weight, slot_token.reshape(EXPERTS, per_expert),
                slot_fill.reshape(EXPERTS, per_expert), slot_weight.reshape(EXPERTS, per_expert))
    hidden_slots, back_slots, grad_mean, grad_rho = lax.map(one_expert, operands)
    picked = jnp.take(hidden_slots.reshape(total, FF), position, axis=0).astype(jnp.float32)
    hidden_out = jnp.sum(picked * route_weight[:, :, None], axis=1).astype(jnp.bfloat16)
    returned = jnp.take(back_slots.reshape(total, D), position, axis=0).astype(jnp.float32)
    grad_tokens = jnp.sum(returned, axis=1).astype(jnp.bfloat16)
    return hidden_out, grad_tokens, grad_mean, grad_rho
```

```python
import functools

import jax
import jax.numpy as jnp
from jax import lax
from jax.experimental import pallas as pl
from jax.experimental.pallas import tpu as pltpu
from jax.sharding import Mesh, PartitionSpec as P


F32 = jnp.float32
BF16 = jnp.bfloat16
I32 = jnp.int32

EXPERTS = 8
CAP = 40
SLOTS = EXPERTS * CAP
TOK = 128
FEAT = 128
FF = 7168
CHIPS = 16
UNIT = FF // (2 * CHIPS)
WORDS = UNIT // 32
HALF_WORDS = CHIPS * WORDS
WIDE = 256
REST = UNIT - 128
PACK = SLOTS * UNIT // 128
FOLD = PACK - SLOTS
TAIL = SLOTS - FOLD
GROUP = 4 * UNIT
GROUPS = FF // GROUP


def iota(shape, dim):
    return lax.broadcasted_iota(I32, shape, dim)


def dot(a, b, dims=((1,), (0,))):
    return lax.dot_general(a, b, (dims, ((), ())), preferred_element_type=F32)


def smem():
    return pl.BlockSpec(memory_space=pltpu.SMEM)


def params(*semantics):
    return pltpu.CompilerParams(
        dimension_semantics=semantics or None, vmem_limit_bytes=48 << 20
    )


def cost(flops, nbytes, trans=0):
    return pl.CostEstimate(flops=flops, bytes_accessed=nbytes, transcendentals=trans)


def ranks_of(ids):
    e = iota((EXPERTS, TOK), 0)
    first = ids[0:1, :] == e
    second = ids[1:2, :] == e
    named = jnp.where(first | second, 1.0, 0.0).astype(BF16)
    before = jnp.where(iota((TOK, TOK), 0) < iota((TOK, TOK), 1), 1.0, 0.0).astype(BF16)
    return first, second, dot(named, before)


def slot_match(mask, rank):
    code = jnp.where(mask, rank, -1.0)
    c = iota((CAP, TOK), 0).astype(F32)
    rows = [
        jnp.where(jnp.broadcast_to(code[e : e + 1, :], (CAP, TOK)) == c, 1.0, 0.0)
        for e in range(EXPERTS)
    ]
    return jnp.concatenate(rows, axis=0)


def sign_bits(words, base):
    lane = iota(words.shape, 1)
    picked = jnp.take_along_axis(
        words, base + lax.shift_right_logical(lane, 5), axis=1, mode="promise_in_bounds"
    )
    return (lax.shift_right_logical(picked, lane & 31) & 1) == 1


def flip(bits, x):
    return jnp.where(bits, -x, x)


def fold(second):
    lane = iota((FOLD, 128), 1)
    tail = second[FOLD:, :]
    moved = [pltpu.roll(tail, (REST - 32 * i) % 128, 1) for i in range(3)]
    return jnp.where(lane < REST, second[:FOLD, :], jnp.concatenate(moved, axis=0))


def unfold(q):
    lane = iota((TAIL, 128), 1)
    r = [pltpu.roll(q[TAIL * i : TAIL * (i + 1), :], 32 * (i + 1), 1) for i in range(3)]
    tail = jnp.where(lane < 32, r[0], jnp.where(lane < 64, r[1], r[2]))
    both = jnp.concatenate([q, tail], axis=0)
    return jnp.where(iota((SLOTS, 128), 1) < REST, both, 0.0)


def dispatch_body(
    core, ids, route, tok, tok_o, ins, ins_o, outs, cot, rows_ref, words_ref, up_ref
):
    c = core[0]
    first, second, rank = ranks_of(ids[...])
    match = slot_match(first | second, rank)
    weight = jnp.where(first, route[0:1, :], jnp.where(second, route[1:2, :], 0.0))
    slot_weight = jnp.concatenate(
        [
            jnp.sum(
                match[CAP * e : CAP * (e + 1), :] * weight[e : e + 1, :], axis=1, keepdims=True
            )
            for e in range(EXPERTS)
        ],
        axis=0,
    )
    hot = match.astype(BF16)
    rows_ref[:, :FEAT] = dot(hot, tok[...]).astype(BF16)
    rows_ref[:, FEAT:] = dot(hot, tok_o[...]).astype(BF16)
    i = iota((HALF_WORDS, FF // 32), 0)
    seventh = lax.shift_right_logical(i * 9363, 16)
    source = 2 * WORDS * seventh + WORDS * c + (i - WORDS * seventh)
    half = jnp.where(iota((HALF_WORDS, FF // 32), 1) == source, 1.0, 0.0).astype(BF16)
    total = jnp.zeros((SLOTS, 128), I32)
    small = jnp.concatenate([ins[...], ins_o[...], jnp.zeros((8, TOK), I32)], axis=0)
    for k in range(4):
        low = (lax.shift_right_logical(outs[...], 8 * k) & 255).astype(F32).astype(BF16)
        kept = dot(half, low)
        rest = (lax.shift_right_logical(small, 8 * k) & 255).astype(F32)
        pieces = jnp.concatenate([kept, rest], axis=0).astype(BF16)
        got = dot(hot, pieces, ((1,), (1,))).astype(I32)
        total = total | lax.shift_left(got, 8 * k)
    words_ref[...] = total
    padded = jnp.concatenate([cot[...], jnp.zeros((WIDE - UNIT, TOK), BF16)], axis=0)
    up_ref[...] = (dot(hot, padded, ((1,), (1,))) * slot_weight).astype(BF16)


def delta_body(core, mean, rho, noise, own_ref, oth_ref):
    c = core[0]
    delta = jnp.log(1.0 + jnp.exp(rho[0].astype(F32))) * noise[0].astype(F32)
    lane = iota((FEAT, WIDE), 1)
    for which, x in ((0, mean[0].astype(F32)), (1, delta)):
        for j in range(4):
            start = UNIT * j
            base = start // 128 * 128
            off = start - base
            width = min(GROUP - base, 384)
            window = x[:, base : base + width]
            if off:
                window = pltpu.roll(window, width - off, 1)
            chunk = jnp.where(lane < UNIT, window[:, :WIDE], 0.0).astype(BF16)

            @pl.when(c == j % 2)
            def _():
                own_ref[which, j // 2] = chunk

            @pl.when(c != j % 2)
            def _():
                oth_ref[which, j // 2] = chunk


def forward_body(words, rows, own, oth, y_ref, signed):
    k = pl.program_id(0)

    @pl.when(k == 0)
    def _():
        for side in range(2):
            bits = sign_bits(words[...], HALF_WORDS + 4 * side)
            a = rows[:, FEAT * side : FEAT * (side + 1)].astype(F32)
            signed[:, FEAT * side : FEAT * (side + 1)] = flip(bits, a).astype(BF16)

    mean = jnp.concatenate([own[0, 0], oth[0, 0]], axis=0)
    delta = jnp.concatenate([own[1, 0], oth[1, 0]], axis=0)
    m = dot(rows[...], mean)
    p = dot(signed[...], delta)
    y1 = m[:, :128] + flip(sign_bits(words[...], WORDS * k), p[:, :128])
    y2 = m[:, 128:] + flip(sign_bits(words[...], WORDS * k + 4), p[:, 128:])
    y_ref[0, :SLOTS, :] = y1.astype(BF16)
    y_ref[0, SLOTS:, :] = fold(y2).astype(BF16)


def middle_body(parts, up, h_ref, dy_ref):
    total = parts[0].astype(F32)
    for i in range(1, CHIPS):
        total = total + parts[i].astype(F32)
    ys = (total[:SLOTS, :], unfold(total[SLOTS:, :]))
    ds = []
    for side, y in enumerate(ys):
        gate = jax.nn.sigmoid(y)
        h_ref[:, 128 * side : 128 * (side + 1)] = (y * gate).astype(BF16)
        u = up[:, 128 * side : 128 * (side + 1)].astype(F32)
        ds.append(u * (gate * (1.0 + y * (1.0 - gate))))
    d1 = ds[0].astype(BF16)
    d2 = fold(ds[1]).astype(BF16)
    for i in range(CHIPS):
        dy_ref[i, :SLOTS, :] = d1
        dy_ref[i, SLOTS:, :] = d2


def backward_body(
    core, words, words_o, rows, dys, dys_o, own, oth, rho, noise,
    gm_ref, gr_ref, g_ref, rows_t, signed_t, acc_m, acc_d,
):
    c = core[0]
    g = pl.program_id(0)

    @pl.when(g == 0)
    def _():
        a = rows[...].astype(F32)
        bits = sign_bits(words[...], HALF_WORDS)
        rows_t[...] = a.T.astype(BF16)
        signed_t[...] = flip(bits, a).T.astype(BF16)
        acc_m[...] = jnp.zeros_like(acc_m)
        acc_d[...] = jnp.zeros_like(acc_d)

    means = []
    deltas = []
    sum_m = acc_m[...]
    sum_d = acc_d[...]
    for kk in range(2):
        for p in range(2):
            mine = c == p
            packed = jnp.where(mine, dys[kk], dys_o[kk]).astype(F32)
            w = jnp.where(mine, words[...], words_o[...])
            base = WORDS * (2 * g + kk)
            d1 = packed[:SLOTS, :]
            d2 = unfold(packed[SLOTS:, :])
            plain = jnp.concatenate([d1, d2], axis=1).astype(BF16)
            signed = jnp.concatenate(
                [flip(sign_bits(w, base), d1), flip(sign_bits(w, base + 4), d2)], axis=1
            ).astype(BF16)
            mean = jnp.where(mine, own[0, kk], oth[0, kk])
            delta = jnp.where(mine, own[1, kk], oth[1, kk])
            sum_m = sum_m + dot(plain, mean, ((1,), (1,)))
            sum_d = sum_d + dot(signed, delta, ((1,), (1,)))
            means.append(dot(rows_t[...], plain)[:, :UNIT])
            deltas.append(dot(signed_t[...], signed)[:, :UNIT])
    acc_m[...] = sum_m
    acc_d[...] = sum_d
    gm_ref[0] = jnp.concatenate(means, axis=1).astype(BF16)
    e = jnp.exp(rho[0].astype(F32))
    factor = noise[0].astype(F32) * (e / (1.0 + e))
    gr_ref[0] = (jnp.concatenate(deltas, axis=1) * factor).astype(BF16)

    @pl.when(g == GROUPS - 1)
    def _():
        bits = sign_bits(words[...], HALF_WORDS)
        g_ref[...] = (acc_m[...] + flip(bits, acc_d[...])).astype(BF16)


def hidden_body(ids, route, h, out_ref):
    first, second, rank = ranks_of(ids[...])
    total = jnp.zeros((WIDE, TOK), F32)
    for k, mask in enumerate((first, second)):
        hot = slot_match(mask, rank).astype(BF16)
        total = total + dot(h[...], hot, ((0,), (0,))) * route[k : k + 1, :]
    out_ref[...] = total[:UNIT, :].astype(BF16)


def tokens_body(ids, g, out_ref):
    first, second, rank = ranks_of(ids[...])
    hot = slot_match(first | second, rank).astype(BF16)
    out_ref[...] = dot(hot, g[...], ((0,), (0,))).astype(BF16)


def whole(*shape):
    return pl.BlockSpec(shape, lambda *_: (0,) * len(shape))


def struct(shape, dtype):
    return jax.ShapeDtypeStruct(shape, dtype)


def on_device(
    tokens, in_signs, out_signs, expert_ids, route_weight, cotangent,
    mean_weight, rho_weight, noise_weight,
):
    core = lax.axis_index("core").astype(I32).reshape(1)
    swap = [(0, 1), (1, 0)]
    ids = expert_ids.T
    route = route_weight.T
    ins = in_signs.T

    tok_o = lax.ppermute(tokens, "core", swap)
    ins_o = lax.ppermute(ins, "core", swap)

    rows, words, up = pl.pallas_call(
        dispatch_body,
        in_specs=[smem()] + [pl.BlockSpec(memory_space=pltpu.VMEM)] * 8,
        out_shape=(
            struct((SLOTS, WIDE), BF16),
            struct((SLOTS, 128), I32),
            struct((SLOTS, WIDE), BF16),
        ),
        compiler_params=params(),
        cost_estimate=cost(400_000_000, 1 << 20),
        name="dispatch",
    )(core, ids, route, tokens, tok_o, ins, ins_o, out_signs.T, cotangent.T)

    def exchange(x):
        wide = x.reshape(EXPERTS, CAP, x.shape[1])
        got = lax.all_to_all(wide, "expert", split_axis=0, concat_axis=0, tiled=True)
        return got.reshape(x.shape)

    rows = exchange(rows)
    words = exchange(words)
    up = exchange(up)

    block = pl.BlockSpec((1, FEAT, GROUP), lambda g: (0, 0, g))
    pair = pl.BlockSpec((2, 2, FEAT, WIDE), lambda g: (0, g, 0, 0))
    own, away = pl.pallas_call(
        delta_body,
        grid=(GROUPS,),
        in_specs=[smem(), block, block, block],
        out_specs=(pair, pair),
        out_shape=(struct((2, CHIPS, FEAT, WIDE), BF16),) * 2,
        compiler_params=params("arbitrary"),
        cost_estimate=cost(2_000_000_000, 10 << 20, 2 * FEAT * FF),
        name="delta",
    )(core, mean_weight, rho_weight, noise_weight)
    near = lax.ppermute(away, "core", swap)

    one = pl.BlockSpec((2, 1, FEAT, WIDE), lambda k: (0, k, 0, 0))
    partial = pl.pallas_call(
        forward_body,
        grid=(CHIPS,),
        in_specs=[whole(SLOTS, 128), whole(SLOTS, WIDE), one, one],
        out_specs=pl.BlockSpec((1, PACK, 128), lambda k: (k, 0, 0)),
        out_shape=struct((CHIPS, PACK, 128), BF16),
        scratch_shapes=[pltpu.VMEM((SLOTS, WIDE), BF16)],
        compiler_params=params("arbitrary"),
        cost_estimate=cost(2_000_000_000, 7 << 20),
        name="forward",
    )(words, rows, own, near)

    def spread(x):
        return lax.all_to_all(x, ("x", "y"), split_axis=0, concat_axis=0, tiled=True)

    parts = spread(partial)
    hidden, copies = pl.pallas_call(
        middle_body,
        out_shape=(struct((SLOTS, WIDE), BF16), struct((CHIPS, PACK, 128), BF16)),
        compiler_params=params(),
        cost_estimate=cost(1_000_000_000, 5 << 20),
        name="middle",
    )(parts, up)
    dys = spread(copies)
    hidden = exchange(hidden)
    words_o = lax.ppermute(words, "core", swap)
    dys_o = lax.ppermute(dys, "core", swap)

    hidden_out = pl.pallas_call(
        hidden_body,
        out_shape=struct((UNIT, TOK), BF16),
        compiler_params=params(),
        cost_estimate=cost(200_000_000, 1 << 19),
        name="combine_hidden",
    )(ids, route, hidden).T

    two = pl.BlockSpec((2, PACK, 128), lambda g: (g, 0, 0))
    grad_mean, grad_rho, grad_slots = pl.pallas_call(
        backward_body,
        grid=(GROUPS,),
        in_specs=[
            smem(), whole(SLOTS, 128), whole(SLOTS, 128),
            pl.BlockSpec((SLOTS, FEAT), lambda g: (0, 0)),
            two, two, pair, pair, block, block,
        ],
        out_specs=(block, block, whole(SLOTS, FEAT)),
        out_shape=(
            struct((1, FEAT, FF), BF16),
            struct((1, FEAT, FF), BF16),
            struct((SLOTS, FEAT), BF16),
        ),
        scratch_shapes=[
            pltpu.VMEM((FEAT, SLOTS), BF16),
            pltpu.VMEM((FEAT, SLOTS), BF16),
            pltpu.VMEM((SLOTS, FEAT), F32),
            pltpu.VMEM((SLOTS, FEAT), F32),
        ],
        compiler_params=params("arbitrary"),
        cost_estimate=cost(5_000_000_000, 16 << 20, FEAT * FF),
        name="backward",
    )(core, words, words_o, rows, dys, dys_o, own, away, rho_weight, noise_weight)

    grad_slots = exchange(grad_slots)
    grad_tokens = pl.pallas_call(
        tokens_body,
        out_shape=struct((TOK, FEAT), BF16),
        compiler_params=params(),
        cost_estimate=cost(100_000_000, 1 << 18),
        name="combine_tokens",
    )(ids, grad_slots)
    return hidden_out, grad_tokens, grad_mean, grad_rho


def solution(mesh):
    fine = Mesh(mesh.devices.reshape(4, 4, 2, 8), ("x", "y", "core", "expert"))
    dp = ("x", "y", "core")
    in_specs = (
        P("expert", dp),
        P("expert", dp),
        P("expert", None),
        P("expert", None),
        P("expert", None),
        P("expert", dp),
        P("expert", dp, None),
        P("expert", dp, None),
        P("expert", dp, None),
    )
    out_specs = (
        P("expert", dp),
        P("expert", dp),
        P("expert", dp, None),
        P("expert", dp, None),
    )
    return jax.shard_map(
        on_device, mesh=fine, in_specs=in_specs, out_specs=out_specs, check_vma=False
    )
```

```python
import functools

import jax
import jax.numpy as jnp
from jax import lax
from jax.experimental import pallas as pl
from jax.experimental.pallas import tpu as pltpu
from jax.sharding import Mesh, PartitionSpec as P


F32 = jnp.float32
BF16 = jnp.bfloat16
I32 = jnp.int32

EXPERTS = 8
CAP = 40
SLOTS = EXPERTS * CAP
TOK = 128
FEAT = 128
FF = 7168
CHIPS = 16
UNIT = FF // (2 * CHIPS)
WORDS = UNIT // 32
HALF_WORDS = CHIPS * WORDS
WIDE = 256
REST = UNIT - 128
PACK = SLOTS * UNIT // 128
FOLD = PACK - SLOTS
TAIL = SLOTS - FOLD
GROUP = 4 * UNIT
GROUPS = FF // GROUP
PER_STEP = 4


def iota(shape, dim):
    return lax.broadcasted_iota(I32, shape, dim)


def dot(a, b, dims=((1,), (0,))):
    return lax.dot_general(a, b, (dims, ((), ())), preferred_element_type=F32)


def smem():
    return pl.BlockSpec(memory_space=pltpu.SMEM)


def params(*semantics):
    return pltpu.CompilerParams(
        dimension_semantics=semantics or None, vmem_limit_bytes=16 << 20
    )


def cost(flops, nbytes, trans=0):
    return pl.CostEstimate(flops=flops, bytes_accessed=nbytes, transcendentals=trans)


def ranks_of(ids):
    e = iota((EXPERTS, TOK), 0)
    first = ids[0:1, :] == e
    second = ids[1:2, :] == e
    named = jnp.where(first | second, 1.0, 0.0).astype(BF16)
    before = jnp.where(iota((TOK, TOK), 0) < iota((TOK, TOK), 1), 1.0, 0.0).astype(BF16)
    return first, second, dot(named, before)


def slot_match(mask, rank):
    code = jnp.where(mask, rank, -1.0)
    c = iota((CAP, TOK), 0).astype(F32)
    rows = [
        jnp.where(jnp.broadcast_to(code[e : e + 1, :], (CAP, TOK)) == c, 1.0, 0.0)
        for e in range(EXPERTS)
    ]
    return jnp.concatenate(rows, axis=0)


def sign_bits(words, base):
    lane = iota(words.shape, 1)
    picked = jnp.take_along_axis(
        words, base + lax.shift_right_logical(lane, 5), axis=1, mode="promise_in_bounds"
    )
    return (lax.shift_right_logical(picked, lane & 31) & 1) == 1


def flip(bits, x):
    return jnp.where(bits, -x, x)


def fold(second):
    lane = iota((FOLD, 128), 1)
    tail = second[FOLD:, :]
    moved = [pltpu.roll(tail, (REST - 32 * i) % 128, 1) for i in range(3)]
    return jnp.where(lane < REST, second[:FOLD, :], jnp.concatenate(moved, axis=0))


def unfold(q):
    lane = iota((TAIL, 128), 1)
    r = [pltpu.roll(q[TAIL * i : TAIL * (i + 1), :], 32 * (i + 1), 1) for i in range(3)]
    tail = jnp.where(lane < 32, r[0], jnp.where(lane < 64, r[1], r[2]))
    both = jnp.concatenate([q, tail], axis=0)
    return jnp.where(iota((SLOTS, 128), 1) < REST, both, 0.0)


def place(lin):
    return (lin >> 6) & 3, (lin >> 4) & 3, (lin >> 3) & 1


def chunk_at(lin, k, l):
    x, y, c = place(lin)
    east = (x + jnp.where(c == 0, l, k)) & 3
    north = (y + jnp.where(c == 0, k, l)) & 3
    return 4 * east + north


def step_of(lin, q, other):
    x, y, c = place(lin)
    dx = (x - (q >> 2)) & 3
    dy = (y - (q & 3)) & 3
    swapped = (c == 0) == bool(other)
    return jnp.where(swapped, 4 * dx + dy, 4 * dy + dx)


def hop(array, steps, first):
    pairs = []
    for x in range(4):
        for y in range(4):
            for c in range(2):
                along_y = (c == 0) == first
                to_x, to_y = (x, (y + steps) % 4) if along_y else ((x + steps) % 4, y)
                pairs.append(((x * 4 + y) * 2 + c, (to_x * 4 + to_y) * 2 + c))
    return lax.ppermute(array, ("x", "y", "core"), pairs)


def dispatch_body(core, ids, route, tok, tok_o, ins, ins_o, outs, cot, send_ref):
    c = core[0]
    first, second, rank = ranks_of(ids[...])
    match = slot_match(first | second, rank)
    weight = jnp.where(first, route[0:1, :], jnp.where(second, route[1:2, :], 0.0))
    slot_weight = jnp.concatenate(
        [
            jnp.sum(
                match[CAP * e : CAP * (e + 1), :] * weight[e : e + 1, :], axis=1, keepdims=True
            )
            for e in range(EXPERTS)
        ],
        axis=0,
    )
    hot = match.astype(BF16)
    send_ref[:, :FEAT] = dot(hot, tok[...]).astype(BF16)
    send_ref[:, FEAT:WIDE] = dot(hot, tok_o[...]).astype(BF16)
    padded = jnp.concatenate([cot[...], jnp.zeros((WIDE - UNIT, TOK), BF16)], axis=0)
    send_ref[:, WIDE : 2 * WIDE] = (dot(hot, padded, ((1,), (1,))) * slot_weight).astype(BF16)
    i = iota((HALF_WORDS, FF // 32), 0)
    seventh = lax.shift_right_logical(i * 9363, 16)
    source = 2 * WORDS * seventh + WORDS * c + (i - WORDS * seventh)
    half = jnp.where(iota((HALF_WORDS, FF // 32), 1) == source, 1.0, 0.0).astype(BF16)
    small = jnp.concatenate([ins[...], ins_o[...], jnp.zeros((8, TOK), I32)], axis=0)
    for k in range(4):
        low = (lax.shift_right_logical(outs[...], 8 * k) & 255).astype(F32).astype(BF16)
        kept = dot(half, low)
        rest = (lax.shift_right_logical(small, 8 * k) & 255).astype(F32)
        pieces = jnp.concatenate([kept, rest], axis=0).astype(BF16)
        at = 2 * WIDE + 128 * k
        send_ref[:, at : at + 128] = dot(hot, pieces, ((1,), (1,))).astype(BF16)


def delta_body(core, mean, rho, noise, own_ref, oth_ref):
    c = core[0]
    delta = jnp.log(1.0 + jnp.exp(rho[0].astype(F32))) * noise[0].astype(F32)
    lane = iota((FEAT, WIDE), 1)
    for which, x in ((0, mean[0].astype(F32)), (1, delta)):
        for j in range(4):
            start = UNIT * j
            base = start // 128 * 128
            off = start - base
            width = min(GROUP - base, 384)
            window = x[:, base : base + width]
            if off:
                window = pltpu.roll(window, width - off, 1)
            chunk = jnp.where(lane < UNIT, window[:, :WIDE], 0.0).astype(BF16)

            @pl.when(c == j % 2)
            def _():
                own_ref[which, j // 2] = chunk

            @pl.when(c != j % 2)
            def _():
                oth_ref[which, j // 2] = chunk


def forward_part(k, lin, rows, signed, words, weights, y_ref):
    for l in range(4):
        mean, delta = (
            jnp.concatenate([weights[l][w, 0], weights[4 + l][w, 0]], axis=0) for w in range(2)
        )
        m = dot(rows, mean)
        p = dot(signed, delta)
        base = WORDS * chunk_at(lin, k, l)
        y1 = m[:, :128] + flip(sign_bits(words, base), p[:, :128])
        y2 = m[:, 128:] + flip(sign_bits(words, base + 4), p[:, 128:])
        y_ref[l, :SLOTS, :] = y1.astype(BF16)
        y_ref[l, SLOTS:, :] = fold(y2).astype(BF16)


def forward_first(k, lin, got, *refs):
    weights, (y_ref, words_ref, signed_ref) = refs[:8], refs[8:]
    words = jnp.zeros((SLOTS, 128), I32)
    for j in range(4):
        at = 2 * WIDE + 128 * j
        plane = got[:, at : at + 128].astype(F32).astype(I32)
        words = words | lax.shift_left(plane, 8 * j)
    words_ref[...] = words
    for side in range(2):
        bits = sign_bits(words, HALF_WORDS + 4 * side)
        a = got[:, FEAT * side : FEAT * (side + 1)].astype(F32)
        signed_ref[:, FEAT * side : FEAT * (side + 1)] = flip(bits, a).astype(BF16)
    forward_part(k, lin[0], got[:, :WIDE], signed_ref[...], words_ref[...], weights, y_ref)


def forward_next(k, lin, rows, signed, words, *refs):
    forward_part(k, lin[0], rows[...], signed[...], words[...], refs[:8], refs[8])


def halfway_body(p0, r1, r2, r3, q0, q1, q2, q3):
    for l, q in enumerate((q0, q1, q2, q3)):
        total = p0[l].astype(F32) + r1[l].astype(F32)
        total = total + (r2[l].astype(F32) + r3[l].astype(F32))
        q[...] = total.astype(q.dtype)


def middle_body(q0, t1, t2, t3, up, h_ref, dy_ref):
    total = q0[...] + t1[...].astype(F32) + (t2[...].astype(F32) + t3[...].astype(F32))
    ys = (total[:SLOTS, :], unfold(total[SLOTS:, :]))
    ds = []
    for side, y in enumerate(ys):
        gate = jax.nn.sigmoid(y)
        h_ref[:, 128 * side : 128 * (side + 1)] = (y * gate).astype(BF16)
        u = up[:, 128 * side : 128 * (side + 1)].astype(F32)
        ds.append(u * (gate * (1.0 + y * (1.0 - gate))))
    dy_ref[:SLOTS, :] = ds[0].astype(BF16)
    dy_ref[SLOTS:, :] = fold(ds[1]).astype(BF16)


def stack_body(a, b, c, d, out_ref):
    for i, x in enumerate((a, b, c, d)):
        out_ref[i] = x[...]


def gradient_chunk(words, dy, k):
    packed = dy.astype(F32)
    d1 = packed[:SLOTS, :]
    d2 = unfold(packed[SLOTS:, :])
    plain = jnp.concatenate([d1, d2], axis=1).astype(BF16)
    signed = jnp.concatenate(
        [
            flip(sign_bits(words, WORDS * k), d1),
            flip(sign_bits(words, WORDS * k + 4), d2),
        ],
        axis=1,
    ).astype(BF16)
    return plain, signed


def gradient_body(lin, words, rows, v0, v1, v2, v3, *refs):
    own, near = refs[:4], refs[4:8]
    mine_ref, theirs_ref, g_ref, g_away_ref, rows_t, signed_t, sum_m, sum_d = refs[8:]
    step = pl.program_id(0)

    @pl.when(step == 0)
    def _():
        for side in range(2):
            lanes = slice(FEAT * side, FEAT * (side + 1))
            a = rows[:, lanes].astype(F32)
            bits = sign_bits(words[...], HALF_WORDS + 4 * side)
            rows_t[lanes, :] = a.T.astype(BF16)
            signed_t[lanes, :] = flip(bits, a).T.astype(BF16)
        sum_m[...] = jnp.zeros_like(sum_m)
        sum_d[...] = jnp.zeros_like(sum_d)

    plains = []
    signeds = []
    for i in range(PER_STEP):
        dy = jnp.where(
            step < 2,
            jnp.where(step == 0, v0[i], v1[i]),
            jnp.where(step == 2, v2[i], v3[i]),
        )
        plain, signed = gradient_chunk(words[...], dy, chunk_at(lin[0], -step, -i))
        plains.append(plain)
        signeds.append(signed)
        for which, g in ((0, dot(rows_t[...], plain)), (1, dot(signed_t[...], signed))):
            mine_ref[which, i] = g[:FEAT, :].astype(BF16)
            theirs_ref[which, i] = g[FEAT:, :].astype(BF16)
    for which, parts, total in ((0, plains, sum_m), (1, signeds, sum_d)):
        weights = jnp.concatenate(
            [
                jnp.concatenate([w[which, 0] for w in side], axis=1)
                for side in (own, near)
            ],
            axis=0,
        )
        total[...] += dot(jnp.concatenate(parts, axis=1), weights, ((1,), (1,)))

    @pl.when(step == pl.num_programs(0) - 1)
    def _():
        for side, ref in ((0, g_ref), (1, g_away_ref)):
            lanes = slice(FEAT * side, FEAT * (side + 1))
            bits = sign_bits(words[...], HALF_WORDS + 4 * side)
            ref[...] = sum_m[:, lanes] + flip(bits, sum_d[:, lanes])


def slots_body(g, g_near, hidden, send_ref):
    send_ref[:, :FEAT] = (g[...] + g_near[...]).astype(BF16)
    send_ref[:, FEAT:] = hidden[...]


def assemble_body(lin, *refs):
    _, _, c = place(lin[0])
    mine, theirs, (rho, noise, gm_ref, gr_ref) = refs[:4], refs[4:8], refs[8:]

    def laid(which, at):
        out = []
        for i in (at, at + 1):
            for p in range(2):
                out.append(jnp.where(c == p, mine[i][which, 0], theirs[i][which, 0])[:, :UNIT])
        return jnp.concatenate([x.astype(F32) for x in out], axis=1)

    for half in range(PER_STEP // 2):
        lanes = slice(GROUP * half, GROUP * (half + 1))
        gm_ref[0, :, lanes] = laid(0, 2 * half).astype(BF16)
        e = jnp.exp(rho[0, :, lanes].astype(F32))
        factor = noise[0, :, lanes].astype(F32) * (e / (1.0 + e))
        gr_ref[0, :, lanes] = (laid(1, 2 * half) * factor).astype(BF16)


def combine_body(ids, route, got, hidden_ref, tokens_ref):
    first, second, rank = ranks_of(ids[...])
    total = jnp.zeros((WIDE, TOK), F32)
    both = jnp.zeros((SLOTS, TOK), F32)
    for k, mask in enumerate((first, second)):
        match = slot_match(mask, rank)
        both = both + match
        picked = dot(got[:, FEAT:], match.astype(BF16), ((0,), (0,)))
        total = total + picked * route[k : k + 1, :]
    hidden_ref[...] = total[:UNIT, :].astype(BF16)
    tokens_ref[...] = dot(both.astype(BF16), got[:, :FEAT], ((0,), (0,))).astype(BF16)


def whole(*shape):
    return pl.BlockSpec(shape, lambda *_: (0,) * len(shape))


def far_memory(*xs):
    return [pltpu.with_memory_space_constraint(x, pltpu.HBM) for x in xs]


def struct(shape, dtype):
    return jax.ShapeDtypeStruct(shape, dtype)


def on_device(
    tokens, in_signs, out_signs, expert_ids, route_weight, cotangent,
    mean_weight, rho_weight, noise_weight,
):
    mean_weight, rho_weight, noise_weight = far_memory(mean_weight, rho_weight, noise_weight)
    core = lax.axis_index("core").astype(I32).reshape(1)
    lin = lax.axis_index(("x", "y", "core", "expert")).astype(I32).reshape(1)
    swap = [(0, 1), (1, 0)]
    ids = expert_ids.T
    route = route_weight.T
    ins = in_signs.T

    tok_o = lax.ppermute(tokens, "core", swap)
    ins_o = lax.ppermute(ins, "core", swap)

    raw = far_memory(ids, route, tokens)
    raw += [tok_o, *far_memory(ins), ins_o, *far_memory(out_signs.T, cotangent.T)]
    send = pl.pallas_call(
        dispatch_body,
        grid=(1,),
        in_specs=[smem()] + [whole(*x.shape) for x in raw],
        out_specs=whole(SLOTS, 4 * WIDE),
        out_shape=struct((SLOTS, 4 * WIDE), BF16),
        compiler_params=params("arbitrary"),
        cost_estimate=cost(400_000_000, 1 << 20),
        name="dispatch",
    )(core, *raw)

    def exchange(x):
        wide = x.reshape(EXPERTS, CAP, x.shape[1])
        got = lax.all_to_all(wide, "expert", split_axis=0, concat_axis=0, tiled=True)
        return got.reshape(x.shape)

    got = exchange(send)

    late, _ = lax.optimization_barrier((core, send))
    block = pl.BlockSpec((1, FEAT, GROUP), lambda g: (0, 0, g))
    pair = pl.BlockSpec((2, 2, FEAT, WIDE), lambda g: (0, g, 0, 0))
    own, away = pl.pallas_call(
        delta_body,
        grid=(GROUPS,),
        in_specs=[smem(), block, block, block],
        out_specs=(pair, pair),
        out_shape=(pltpu.HBM((2, CHIPS, FEAT, WIDE), BF16),) * 2,
        compiler_params=params("arbitrary"),
        cost_estimate=cost(2_000_000_000, 10 << 20, 2 * FEAT * FF),
        name="delta",
    )(late, mean_weight, rho_weight, noise_weight)
    near = lax.ppermute(away, "core", swap)

    steps = CHIPS // PER_STEP
    table = whole(SLOTS, 128)
    rows_spec = pl.BlockSpec((SLOTS, WIDE), lambda *_: (0, 0))
    quad = struct((4, PACK, 128), BF16)
    quad_spec = whole(4, PACK, 128)
    lone_spec = whole(PACK, 128)

    def picked(index):
        return pl.BlockSpec(
            (2, 1, FEAT, WIDE), lambda i, lin: (0, index(lin[0], i), 0, 0)
        )

    def grid_spec(n, ins, outs, scratch=()):
        return pltpu.PrefetchScalarGridSpec(
            num_scalar_prefetch=1, grid=(n,), in_specs=ins, out_specs=outs,
            scratch_shapes=scratch,
        )

    sent = [None] * 4
    words = signed = None
    for k in (1, 3, 2, 0):
        chunks = [
            picked(lambda lin, i, k=k, l=l: chunk_at(lin, k, l)) for l in range(4)
        ] * 2
        if words is None:
            sent[k], words, signed = pl.pallas_call(
                functools.partial(forward_first, k),
                grid_spec=grid_spec(
                    1, [whole(SLOTS, 4 * WIDE), *chunks], (quad_spec, table, rows_spec)
                ),
                out_shape=(quad, struct((SLOTS, 128), I32), struct((SLOTS, WIDE), BF16)),
                compiler_params=params("arbitrary"),
                cost_estimate=cost(600_000_000, 2 << 20),
            )(lin, got, *[own] * 4, *[near] * 4)
        else:
            sent[k] = pl.pallas_call(
                functools.partial(forward_next, k),
                grid_spec=grid_spec(1, [rows_spec, rows_spec, table, *chunks], quad_spec),
                out_shape=quad,
                compiler_params=params("arbitrary"),
                cost_estimate=cost(600_000_000, 2 << 20),
            )(lin, got, signed, words, *[own] * 4, *[near] * 4)
    parts = [sent[0]] + [hop(sent[k], k, True) for k in (1, 2, 3)]
    lone = struct((PACK, 128), BF16)
    kept, *passed = pl.pallas_call(
        halfway_body,
        grid=(1,),
        in_specs=[quad_spec] * 4,
        out_specs=(lone_spec,) * 4,
        out_shape=(struct((PACK, 128), F32), lone, lone, lone),
        compiler_params=params("arbitrary"),
        cost_estimate=cost(200_000_000, 3 << 20),
        name="halfway",
    )(*parts)
    passed = [hop(passed[l - 1], l, False) for l in (1, 2, 3)]
    hidden, dy = pl.pallas_call(
        middle_body,
        grid=(1,),
        in_specs=[lone_spec] * 4 + [pl.BlockSpec((SLOTS, WIDE), lambda *_: (0, 1))],
        out_specs=(whole(SLOTS, WIDE), lone_spec),
        out_shape=(struct((SLOTS, WIDE), BF16), lone),
        compiler_params=params("arbitrary"),
        cost_estimate=cost(200_000_000, 1 << 20),
        name="middle",
    )(kept, *passed, got)
    stack = pl.pallas_call(
        stack_body,
        grid=(1,),
        in_specs=[lone_spec] * 4,
        out_specs=quad_spec,
        out_shape=quad,
        compiler_params=params("arbitrary"),
        cost_estimate=cost(100_000_000, 1 << 20),
        name="stack",
    )(dy, *[hop(dy, l, False) for l in (1, 2, 3)])
    dys = [stack] + [hop(stack, k, True) for k in (1, 2, 3)]

    sums = whole(SLOTS, FEAT)
    side = pltpu.HBM((2, CHIPS, FEAT, WIDE), BF16)
    weights = pl.BlockSpec((2, PER_STEP, FEAT, WIDE), lambda k, lin: (0, k, 0, 0))
    chunks = [picked(lambda lin, i, l=l: chunk_at(lin, -i, -l)) for l in range(4)] * 2
    mine, theirs, g, g_away = pl.pallas_call(
        gradient_body,
        grid_spec=grid_spec(
            steps,
            [table, rows_spec] + [quad_spec] * 4 + chunks,
            (weights, weights, sums, sums),
            [pltpu.VMEM((WIDE, SLOTS), BF16)] * 2 + [pltpu.VMEM((SLOTS, WIDE), F32)] * 2,
        ),
        out_shape=(side, side, struct((SLOTS, FEAT), F32), struct((SLOTS, FEAT), F32)),
        compiler_params=params("arbitrary"),
        cost_estimate=cost(5_000_000_000, 12 << 20),
        name="backward",
    )(lin, words, got, *dys, *[own] * 4, *[near] * 4)
    g_near = lax.ppermute(g_away, "core", swap)
    theirs, _ = lax.optimization_barrier((theirs, g_near))
    theirs = lax.ppermute(theirs, "core", swap)
    send = pl.pallas_call(
        slots_body,
        grid=(1,),
        in_specs=[sums, sums, whole(SLOTS, WIDE)],
        out_specs=whole(SLOTS, FEAT + WIDE),
        out_shape=struct((SLOTS, FEAT + WIDE), BF16),
        compiler_params=params("arbitrary"),
        cost_estimate=cost(100_000_000, 1 << 20),
        name="slots",
    )(g, g_near, hidden)
    back = exchange(send)
    late, _ = lax.optimization_barrier((lin, send))
    wide = pl.BlockSpec((1, FEAT, FF // steps), lambda g, lin: (0, 0, g))
    laid = [
        picked(lambda lin, i, l=l, other=other: step_of(lin, 4 * i + l, other))
        for other in range(2)
        for l in range(4)
    ]
    grad_mean, grad_rho = pl.pallas_call(
        assemble_body,
        grid_spec=grid_spec(steps, [*laid, wide, wide], (wide, wide)),
        out_shape=(struct((1, FEAT, FF), BF16),) * 2,
        compiler_params=params("arbitrary"),
        cost_estimate=cost(3_000_000_000, 12 << 20, FEAT * FF),
        name="assemble",
    )(late, *[mine] * 4, *[theirs] * 4, rho_weight, noise_weight)

    hidden_out, grad_tokens = pl.pallas_call(
        combine_body,
        grid=(1,),
        in_specs=[whole(2, TOK), whole(2, TOK), whole(SLOTS, FEAT + WIDE)],
        out_specs=(whole(UNIT, TOK), whole(TOK, FEAT)),
        out_shape=(struct((UNIT, TOK), BF16), struct((TOK, FEAT), BF16)),
        compiler_params=params("arbitrary"),
        cost_estimate=cost(200_000_000, 1 << 19),
        name="combine",
    )(*far_memory(ids, route), back)
    return hidden_out.T, grad_tokens, grad_mean, grad_rho


def solution(mesh):
    fine = Mesh(mesh.devices.reshape(4, 4, 2, 8), ("x", "y", "core", "expert"))
    dp = ("x", "y", "core")
    in_specs = (
        P("expert", dp),
        P("expert", dp),
        P("expert", None),
        P("expert", None),
        P("expert", None),
        P("expert", dp),
        P("expert", dp, None),
        P("expert", dp, None),
        P("expert", dp, None),
    )
    out_specs = (
        P("expert", dp),
        P("expert", dp),
        P("expert", dp, None),
        P("expert", dp, None),
    )

    return jax.shard_map(
        on_device, mesh=fine, in_specs=in_specs, out_specs=out_specs, check_vma=False
    )
```

```python
import functools

import jax
import jax.numpy as jnp
from jax import lax
from jax.experimental import pallas as pl
from jax.experimental.pallas import tpu as pltpu
from jax.sharding import Mesh, PartitionSpec as P


F32 = jnp.float32
BF16 = jnp.bfloat16
I32 = jnp.int32

EXPERTS = 8
CAP = 40
SLOTS = EXPERTS * CAP
TOK = 128
FEAT = 128
FF = 7168
CHIPS = 16
UNIT = FF // (2 * CHIPS)
WORDS = UNIT // 32
HALF_WORDS = CHIPS * WORDS
WIDE = 256
REST = UNIT - 128
PACK = SLOTS * UNIT // 128
FOLD = PACK - SLOTS
TAIL = SLOTS - FOLD
GROUP = 4 * UNIT
GROUPS = FF // GROUP
PER_STEP = 4
FLAG = 1
DELTA_GROUPS = 2


def iota(shape, dim):
    return lax.broadcasted_iota(I32, shape, dim)


def dot(a, b, dims=((1,), (0,))):
    return lax.dot_general(a, b, (dims, ((), ())), preferred_element_type=F32)


def smem():
    return pl.BlockSpec(memory_space=pltpu.SMEM)


def params(*semantics):
    return pltpu.CompilerParams(
        dimension_semantics=semantics or None, vmem_limit_bytes=16 << 20
    )


def cost(flops, nbytes, trans=0):
    return pl.CostEstimate(flops=flops, bytes_accessed=nbytes, transcendentals=trans)


def ranks_of(ids):
    e = iota((EXPERTS, TOK), 0)
    first = ids[0:1, :] == e
    second = ids[1:2, :] == e
    named = jnp.where(first | second, 1.0, 0.0).astype(BF16)
    before = jnp.where(iota((TOK, TOK), 0) < iota((TOK, TOK), 1), 1.0, 0.0).astype(BF16)
    return first, second, dot(named, before)


def slot_match(mask, rank):
    code = jnp.where(mask, rank, -1.0)
    c = iota((CAP, TOK), 0).astype(F32)
    rows = [
        jnp.where(jnp.broadcast_to(code[e : e + 1, :], (CAP, TOK)) == c, 1.0, 0.0)
        for e in range(EXPERTS)
    ]
    return jnp.concatenate(rows, axis=0)


def sign_bits(words, base):
    lane = iota(words.shape, 1)
    picked = jnp.take_along_axis(
        words, base + lax.shift_right_logical(lane, 5), axis=1, mode="promise_in_bounds"
    )
    return (lax.shift_right_logical(picked, lane & 31) & 1) == 1


def flip(bits, x):
    return jnp.where(bits, -x, x)


def fold(second):
    lane = iota((FOLD, 128), 1)
    tail = second[FOLD:, :]
    moved = [pltpu.roll(tail, (REST - 32 * i) % 128, 1) for i in range(3)]
    return jnp.where(lane < REST, second[:FOLD, :], jnp.concatenate(moved, axis=0))


def unfold(q):
    lane = iota((TAIL, 128), 1)
    r = [pltpu.roll(q[TAIL * i : TAIL * (i + 1), :], 32 * (i + 1), 1) for i in range(3)]
    tail = jnp.where(lane < 32, r[0], jnp.where(lane < 64, r[1], r[2]))
    both = jnp.concatenate([q, tail], axis=0)
    return jnp.where(iota((SLOTS, 128), 1) < REST, both, 0.0)


def place(lin):
    return (lin >> 6) & 3, (lin >> 4) & 3, (lin >> 3) & 1


def chunk_at(lin, k, l):
    x, y, c = place(lin)
    east = (x + jnp.where(c == 0, l, k)) & 3
    north = (y + jnp.where(c == 0, k, l)) & 3
    return 4 * east + north


def step_of(lin, q, other):
    x, y, c = place(lin)
    dx = (x - (q >> 2)) & 3
    dy = (y - (q & 3)) & 3
    swapped = (c == 0) == bool(other)
    return jnp.where(swapped, 4 * dx + dy, 4 * dy + dx)


def hop(array, steps, first):
    pairs = []
    for x in range(4):
        for y in range(4):
            for c in range(2):
                along_y = (c == 0) == first
                to_x, to_y = (x, (y + steps) % 4) if along_y else ((x + steps) % 4, y)
                pairs.append(((x * 4 + y) * 2 + c, (to_x * 4 + to_y) * 2 + c))
    return lax.ppermute(array, ("x", "y", "core"), pairs)


def dispatch_body(core, ids, route, tok, tok_o, ins, ins_o, outs, cot, send_ref):
    c = core[0]
    first, second, rank = ranks_of(ids[...])
    match = slot_match(first | second, rank)
    weight = jnp.where(first, route[0:1, :], jnp.where(second, route[1:2, :], 0.0))
    slot_weight = jnp.concatenate(
        [
            jnp.sum(
                match[CAP * e : CAP * (e + 1), :] * weight[e : e + 1, :], axis=1, keepdims=True
            )
            for e in range(EXPERTS)
        ],
        axis=0,
    )
    hot = match.astype(BF16)
    send_ref[:, :FEAT] = dot(hot, tok[...]).astype(BF16)
    send_ref[:, FEAT:WIDE] = dot(hot, tok_o[...]).astype(BF16)
    padded = jnp.concatenate([cot[...], jnp.zeros((WIDE - UNIT, TOK), BF16)], axis=0)
    send_ref[:, WIDE : 2 * WIDE] = (dot(hot, padded, ((1,), (1,))) * slot_weight).astype(BF16)
    i = iota((HALF_WORDS, FF // 32), 0)
    seventh = lax.shift_right_logical(i * 9363, 16)
    source = 2 * WORDS * seventh + WORDS * c + (i - WORDS * seventh)
    half = jnp.where(iota((HALF_WORDS, FF // 32), 1) == source, 1.0, 0.0).astype(BF16)
    small = jnp.concatenate([ins[...], ins_o[...], jnp.zeros((8, TOK), I32)], axis=0)
    for k in range(4):
        low = (lax.shift_right_logical(outs[...], 8 * k) & 255).astype(F32).astype(BF16)
        kept = dot(half, low)
        rest = (lax.shift_right_logical(small, 8 * k) & 255).astype(F32)
        pieces = jnp.concatenate([kept, rest], axis=0).astype(BF16)
        at = 2 * WIDE + 128 * k
        send_ref[:, at : at + 128] = dot(hot, pieces, ((1,), (1,))).astype(BF16)


def delta_body(core, mean, rho, noise, own_ref, oth_ref):
    c = core[0]
    lane = iota((FEAT, WIDE), 1)
    for g in range(DELTA_GROUPS):
        lanes = slice(GROUP * g, GROUP * (g + 1))
        u = jnp.exp(rho[0, :, lanes].astype(F32))
        delta = jnp.log(1.0 + u) * noise[0, :, lanes].astype(F32)
        for which, x in ((0, mean[0, :, lanes].astype(F32)), (1, delta)):
            for j in range(4):
                start = UNIT * j
                base = start // 128 * 128
                off = start - base
                width = min(GROUP - base, 384)
                window = x[:, base : base + width]
                if off:
                    window = pltpu.roll(window, width - off, 1)
                chunk = jnp.where(lane < UNIT, window[:, :WIDE], 0.0).astype(BF16)
                at = 2 * g + j // 2

                @pl.when(c == j % 2)
                def _():
                    own_ref[which, at] = chunk

                @pl.when(c != j % 2)
                def _():
                    oth_ref[which, at] = chunk


def forward_part(k, lin, rows, signed, words, weights, halves):
    for l in range(4):
        mean, delta = (
            jnp.concatenate([weights[l][w, 0], weights[4 + l][w, 0]], axis=0) for w in range(2)
        )
        m = dot(rows, mean)
        p = dot(signed, delta)
        base = WORDS * chunk_at(lin, k, l)
        y1 = m[:, :128] + flip(sign_bits(words, base), p[:, :128])
        y2 = m[:, 128:] + flip(sign_bits(words, base + 4), p[:, 128:])
        halves[l // 2][l % 2, :SLOTS, :] = y1.astype(BF16)
        halves[l // 2][l % 2, SLOTS:, :] = fold(y2).astype(BF16)


def forward_first(k, lin, got, *refs):
    weights, halves, (words_ref, signed_ref) = refs[:8], refs[8:10], refs[10:]
    words = jnp.zeros((SLOTS, 128), I32)
    for j in range(4):
        at = 2 * WIDE + 128 * j
        plane = got[:, at : at + 128].astype(F32).astype(I32)
        words = words | lax.shift_left(plane, 8 * j)
    words_ref[...] = words
    for side in range(2):
        bits = sign_bits(words, HALF_WORDS + 4 * side)
        a = got[:, FEAT * side : FEAT * (side + 1)].astype(F32)
        signed_ref[:, FEAT * side : FEAT * (side + 1)] = flip(bits, a).astype(BF16)
    forward_part(k, lin[0], got[:, :WIDE], signed_ref[...], words_ref[...], weights, halves)


def forward_next(k, lin, rows, signed, words, *refs):
    forward_part(k, lin[0], rows[...], signed[...], words[...], refs[:8], refs[8:10])


def join_body(a, b, out_ref):
    out_ref[...] = (a[...].astype(F32) + b[...].astype(F32)).astype(BF16)


def halfway_body(low, low1, low3, high, high1, high3, q0, q1, q2, q3):
    for l, q in enumerate((q0, q1, q2, q3)):
        a, b, c = ((low, low1, low3), (high, high1, high3))[l // 2]
        i = l % 2
        total = a[i].astype(F32) + b[i].astype(F32) + c[i].astype(F32)
        q[...] = total.astype(q.dtype)


def middle_body(q0, t1, t2, t3, up, h_ref, dy_ref):
    total = q0[...] + t1[...].astype(F32) + (t2[...].astype(F32) + t3[...].astype(F32))
    ys = (total[:SLOTS, :], unfold(total[SLOTS:, :]))
    ds = []
    for side, y in enumerate(ys):
        gate = jax.nn.sigmoid(y)
        h_ref[:, 128 * side : 128 * (side + 1)] = (y * gate).astype(BF16)
        u = up[:, 128 * side : 128 * (side + 1)].astype(F32)
        ds.append(u * (gate * (1.0 + y * (1.0 - gate))))
    dy_ref[:SLOTS, :] = ds[0].astype(BF16)
    dy_ref[SLOTS:, :] = fold(ds[1]).astype(BF16)


def stack_body(a, b, c, d, _, low_ref, high_ref):
    for i, x in enumerate((a, b, c, d)):
        (low_ref, high_ref)[i // 2][i % 2] = x[...]


def gradient_chunk(words, dy, k):
    packed = dy.astype(F32)
    d1 = packed[:SLOTS, :]
    d2 = unfold(packed[SLOTS:, :])
    plain = jnp.concatenate([d1, d2], axis=1).astype(BF16)
    signed = jnp.concatenate(
        [
            flip(sign_bits(words, WORDS * k), d1),
            flip(sign_bits(words, WORDS * k + 4), d2),
        ],
        axis=1,
    ).astype(BF16)
    return plain, signed


def gradient_part(k, lin, words, rows_t, signed_t, dys, weights, sums, mine_ref, theirs_ref):
    plains = []
    signeds = []
    for l in range(4):
        dy = dys[l // 2][l % 2]
        plain, signed = gradient_chunk(words, dy, chunk_at(lin, -k, -l))
        plains.append(plain)
        signeds.append(signed)
        for which, g in ((0, dot(rows_t, plain)), (1, dot(signed_t, signed))):
            mine_ref[which, l] = g[:FEAT, :].astype(BF16)
            theirs_ref[which, l] = g[FEAT:, :].astype(BF16)
    out = []
    for which, parts in ((0, plains), (1, signeds)):
        side = [
            jnp.concatenate([w[which, 0] for w in weights[at : at + 4]], axis=1) for at in (0, 4)
        ]
        total = dot(
            jnp.concatenate(parts, axis=1), jnp.concatenate(side, axis=0), ((1,), (1,))
        )
        out.append(total if sums is None else total + sums[which][...])
    return out


def gradient_first(lin, words, rows, low, high, *refs):
    dys = (low, high)
    weights, (mine, theirs, rows_t, signed_t, sum_m, sum_d) = refs[:8], refs[8:]
    for side in range(2):
        lanes = slice(FEAT * side, FEAT * (side + 1))
        a = rows[:, lanes].astype(F32)
        bits = sign_bits(words[...], HALF_WORDS + 4 * side)
        rows_t[lanes, :] = a.T.astype(BF16)
        signed_t[lanes, :] = flip(bits, a).T.astype(BF16)
    sum_m[...], sum_d[...] = gradient_part(
        0, lin[0], words[...], rows_t[...], signed_t[...], dys, weights, None, mine, theirs
    )


def gradient_next(k, lin, words, rows_t, signed_t, in_m, in_d, low, high, *refs):
    dys = (low, high)
    weights, (_, _, mine, theirs, sum_m, sum_d) = refs[:8], refs[8:]
    sum_m[...], sum_d[...] = gradient_part(
        k, lin[0], words[...], rows_t[...], signed_t[...], dys, weights, (in_m, in_d),
        mine, theirs,
    )


def gradient_last(k, lin, words, rows_t, signed_t, in_m, in_d, low, high, *refs):
    dys = (low, high)
    weights, (_, _, mine, theirs, g_ref, g_away_ref) = refs[:8], refs[8:]
    total_m, total_d = gradient_part(
        k, lin[0], words[...], rows_t[...], signed_t[...], dys, weights, (in_m, in_d),
        mine, theirs,
    )
    for side, ref in ((0, g_ref), (1, g_away_ref)):
        lanes = slice(FEAT * side, FEAT * (side + 1))
        bits = sign_bits(words[...], HALF_WORDS + 4 * side)
        ref[...] = total_m[:, lanes] + flip(bits, total_d[:, lanes])


def slots_body(g, g_near, hidden, send_ref):
    send_ref[:, :FEAT] = (g[...] + g_near[...]).astype(BF16)
    send_ref[:, FEAT:] = hidden[...]


def assemble_body(lin, *refs):
    _, _, c = place(lin[0])
    mine, theirs, (rho, noise, gm_ref, gr_ref) = refs[:4], refs[4:8], refs[8:]

    def laid(which, at):
        out = []
        for i in (at, at + 1):
            for p in range(2):
                out.append(jnp.where(c == p, mine[i][which, 0], theirs[i][which, 0])[:, :UNIT])
        return jnp.concatenate([x.astype(F32) for x in out], axis=1)

    for half in range(PER_STEP // 2):
        lanes = slice(GROUP * half, GROUP * (half + 1))
        gm_ref[0, :, lanes] = laid(0, 2 * half).astype(BF16)
        e = jnp.exp(rho[0, :, lanes].astype(F32))
        factor = noise[0, :, lanes].astype(F32) * (e / (1.0 + e))
        gr_ref[0, :, lanes] = (laid(1, 2 * half) * factor).astype(BF16)


def combine_body(ids, route, got, hidden_ref, tokens_ref):
    first, second, rank = ranks_of(ids[...])
    total = jnp.zeros((WIDE, TOK), F32)
    both = jnp.zeros((SLOTS, TOK), F32)
    for k, mask in enumerate((first, second)):
        match = slot_match(mask, rank)
        both = both + match
        picked = dot(got[:, FEAT:], match.astype(BF16), ((0,), (0,)))
        total = total + picked * route[k : k + 1, :]
    hidden_ref[...] = total[:UNIT, :].astype(BF16)
    tokens_ref[...] = dot(both.astype(BF16), got[:, :FEAT], ((0,), (0,))).astype(BF16)


def whole(*shape):
    return pl.BlockSpec(shape, lambda *_: (0,) * len(shape))


def far_memory(*xs):
    return [pltpu.with_memory_space_constraint(x, pltpu.HBM) for x in xs]


def struct(shape, dtype):
    return jax.ShapeDtypeStruct(shape, dtype)


def on_device(
    tokens, in_signs, out_signs, expert_ids, route_weight, cotangent,
    mean_weight, rho_weight, noise_weight,
):
    mean_weight, rho_weight, noise_weight = far_memory(mean_weight, rho_weight, noise_weight)
    core = lax.axis_index("core").astype(I32).reshape(1)
    lin = lax.axis_index(("x", "y", "core", "expert")).astype(I32).reshape(1)
    swap = [(0, 1), (1, 0)]
    ids = expert_ids.T
    route = route_weight.T
    ins = in_signs.T

    tok_o = lax.ppermute(tokens, "core", swap)
    ins_o = lax.ppermute(ins, "core", swap)

    raw = far_memory(ids, route, tokens)
    raw += [tok_o, *far_memory(ins), ins_o, *far_memory(out_signs.T, cotangent.T)]
    send = pl.pallas_call(
        dispatch_body,
        grid=(1,),
        in_specs=[smem()] + [whole(*x.shape) for x in raw],
        out_specs=whole(SLOTS, 4 * WIDE),
        out_shape=struct((SLOTS, 4 * WIDE), BF16),
        compiler_params=params("arbitrary"),
        cost_estimate=cost(400_000_000, 1 << 20),
        name="dispatch",
    )(core, *raw)

    def exchange(x):
        wide = x.reshape(EXPERTS, CAP, x.shape[1])
        got = lax.all_to_all(wide, "expert", split_axis=0, concat_axis=0, tiled=True)
        return got.reshape(x.shape)

    got = exchange(send)

    late, _ = lax.optimization_barrier((core, send))
    block = pl.BlockSpec((1, FEAT, DELTA_GROUPS * GROUP), lambda g: (0, 0, g))
    pair = pl.BlockSpec((2, 2 * DELTA_GROUPS, FEAT, WIDE), lambda g: (0, g, 0, 0))
    own, away = pl.pallas_call(
        delta_body,
        grid=(GROUPS // DELTA_GROUPS,),
        in_specs=[smem(), block, block, block],
        out_specs=(pair, pair),
        out_shape=(pltpu.HBM((2, CHIPS, FEAT, WIDE), BF16),) * 2,
        compiler_params=params("arbitrary"),
        cost_estimate=cost(2_000_000_000, 10 << 20, 2 * FEAT * FF),
        name="delta",
    )(late, mean_weight, rho_weight, noise_weight)
    near = lax.ppermute(away, "core", swap)

    steps = CHIPS // PER_STEP
    table = whole(SLOTS, 128)
    rows_spec = pl.BlockSpec((SLOTS, WIDE), lambda *_: (0, 0))
    half = struct((2, PACK, 128), BF16)
    half_spec = whole(2, PACK, 128)
    lone_spec = whole(PACK, 128)

    def picked(index):
        return pl.BlockSpec(
            (2, 1, FEAT, WIDE), lambda i, lin: (0, index(lin[0], i), 0, 0)
        )

    def grid_spec(n, ins, outs, scratch=()):
        return pltpu.PrefetchScalarGridSpec(
            num_scalar_prefetch=1, grid=(n,), in_specs=ins, out_specs=outs,
            scratch_shapes=scratch,
        )

    (own_far,) = far_memory(own)
    sent = [[] for _ in range(4)]
    words = signed = None
    for k in (2, 1, 3, 0):
        chunks = [
            picked(lambda lin, i, k=k, l=l: chunk_at(lin, k, l)) for l in range(4)
        ] * 2
        if words is None:
            *sent[k], words, signed = pl.pallas_call(
                functools.partial(forward_first, k),
                grid_spec=grid_spec(
                    1, [whole(SLOTS, 4 * WIDE), *chunks], (half_spec, half_spec, table, rows_spec)
                ),
                out_shape=(
                    half, half, struct((SLOTS, 128), I32), struct((SLOTS, WIDE), BF16)
                ),
                compiler_params=params("arbitrary"),
                cost_estimate=cost(600_000_000, 2 << 20),
            )(lin, got, *[own_far] * 4, *[near] * 4)
        else:
            sent[k] = pl.pallas_call(
                functools.partial(forward_next, k),
                grid_spec=grid_spec(
                    1, [rows_spec, rows_spec, table, *chunks], (half_spec, half_spec)
                ),
                out_shape=(half, half),
                compiler_params=params("arbitrary"),
                cost_estimate=cost(600_000_000, 2 << 20),
            )(lin, got, signed, words, *[own] * 4, *[near] * 4)

    def move(x, steps):
        return hop(x, steps, True)

    def joined(x, y):
        return pl.pallas_call(
            join_body,
            grid=(1,),
            in_specs=[half_spec, half_spec],
            out_specs=half_spec,
            out_shape=half,
            compiler_params=params("arbitrary"),
            cost_estimate=cost(50_000_000, 1 << 20),
        )(x, y)

    from_below = move(sent[2][0], 1)
    from_above = move(sent[2][1], 3)
    high1 = move(sent[1][1], 1)
    low3 = move(sent[3][0], 3)
    low1 = move(joined(sent[1][0], from_below), 1)
    high3 = move(joined(sent[3][1], from_above), 3)
    lone = struct((PACK, 128), BF16)
    kept, *passed = pl.pallas_call(
        halfway_body,
        grid=(1,),
        in_specs=[half_spec] * 6,
        out_specs=(lone_spec,) * 4,
        out_shape=(struct((PACK, 128), F32), lone, lone, lone),
        compiler_params=params("arbitrary"),
        cost_estimate=cost(200_000_000, 3 << 20),
        name="halfway",
    )(sent[0][0], low1, low3, sent[0][1], high1, high3)
    passed = [hop(passed[l - 1], l, False) for l in (1, 2, 3)]
    hidden, dy = pl.pallas_call(
        middle_body,
        grid=(1,),
        in_specs=[lone_spec] * 4 + [pl.BlockSpec((SLOTS, WIDE), lambda *_: (0, 1))],
        out_specs=(whole(SLOTS, WIDE), lone_spec),
        out_shape=(struct((SLOTS, WIDE), BF16), lone),
        compiler_params=params("arbitrary"),
        cost_estimate=cost(200_000_000, 1 << 20),
        name="middle",
    )(kept, *passed, got)
    beside = [hop(dy, l, False) for l in (1, 2, 3)]
    partner = lax.ppermute(beside[FLAG], "core", swap)
    low, high = pl.pallas_call(
        stack_body,
        grid=(1,),
        in_specs=[lone_spec] * 4 + [pl.BlockSpec(memory_space=pl.ANY)],
        out_specs=(half_spec, half_spec),
        out_shape=(half, half),
        compiler_params=params("arbitrary"),
        cost_estimate=cost(100_000_000, 1 << 20),
        name="stack",
    )(dy, *beside, partner)
    low1 = move(low, 1)
    high3 = move(high, 3)
    high1 = move(high, 1)
    low3 = move(low, 3)
    low2 = move(low1, 1)
    high2 = move(high3, 3)
    dys = [(low, high), (low1, high1), (low2, high2), (low3, high3)]

    sums = whole(SLOTS, FEAT)
    wide_sums = whole(SLOTS, WIDE)
    turned = whole(WIDE, SLOTS)
    side = pltpu.HBM((2, CHIPS, FEAT, WIDE), BF16)
    in_place = pl.BlockSpec(memory_space=pltpu.HBM)
    turned_shape = struct((WIDE, SLOTS), BF16)
    total_shape = struct((SLOTS, WIDE), F32)
    slot_shape = struct((SLOTS, FEAT), F32)
    for k in (0, 1, 3, 2):
        chunks = [
            picked(lambda lin, i, k=k, l=l: chunk_at(lin, -k, -l)) for l in range(4)
        ] * 2
        block = pl.BlockSpec((2, 4, FEAT, WIDE), lambda i, lin, k=k: (0, k, 0, 0))
        last = k == 2
        if k == 0:
            body = gradient_first
            ins = [table, rows_spec, half_spec, half_spec, *chunks]
            outs = (turned, turned, wide_sums, wide_sums)
            shapes = (turned_shape, turned_shape, total_shape, total_shape)
            operands = (words, got, *dys[k])
            carried = ()
        else:
            body = functools.partial(gradient_last if last else gradient_next, k)
            ins = [table, turned, turned, wide_sums, wide_sums, half_spec, half_spec, *chunks]
            ins += [in_place, in_place]
            outs = (sums, sums) if last else (wide_sums, wide_sums)
            shapes = (slot_shape,) * 2 if last else (total_shape,) * 2
            operands = (words, rows_t, signed_t, *totals, *dys[k])
            carried = (mine, theirs)
        got_back = pl.pallas_call(
            body,
            grid_spec=grid_spec(1, ins, (block, block, *outs)),
            out_shape=(side, side, *shapes),
            input_output_aliases={len(ins) - 1: 0, len(ins): 1} if carried else {},
            compiler_params=params("arbitrary"),
            cost_estimate=cost(1_300_000_000, 3 << 20),
        )(lin, *operands, *[own] * 4, *[near] * 4, *carried)
        mine, theirs, *rest = got_back
        if k == 0:
            rows_t, signed_t, *rest = rest
        totals = rest
    g, g_away = totals
    g_near = lax.ppermute(g_away, "core", swap)
    theirs, _ = lax.optimization_barrier((theirs, g_near))
    theirs = lax.ppermute(theirs, "core", swap)
    send = pl.pallas_call(
        slots_body,
        grid=(1,),
        in_specs=[sums, sums, whole(SLOTS, WIDE)],
        out_specs=whole(SLOTS, FEAT + WIDE),
        out_shape=struct((SLOTS, FEAT + WIDE), BF16),
        compiler_params=params("arbitrary"),
        cost_estimate=cost(100_000_000, 1 << 20),
        name="slots",
    )(g, g_near, hidden)
    back = exchange(send)
    late, _ = lax.optimization_barrier((lin, send))
    wide = pl.BlockSpec((1, FEAT, FF // steps), lambda g, lin: (0, 0, g))
    laid = [
        picked(lambda lin, i, l=l, other=other: step_of(lin, 4 * i + l, other))
        for other in range(2)
        for l in range(4)
    ]
    grad_mean, grad_rho = pl.pallas_call(
        assemble_body,
        grid_spec=grid_spec(steps, [*laid, wide, wide], (wide, wide)),
        out_shape=(struct((1, FEAT, FF), BF16),) * 2,
        compiler_params=params("arbitrary"),
        cost_estimate=cost(3_000_000_000, 12 << 20, FEAT * FF),
        name="assemble",
    )(late, *far_memory(*[mine] * 4), *[theirs] * 4, rho_weight, noise_weight)

    hidden_out, grad_tokens = pl.pallas_call(
        combine_body,
        grid=(1,),
        in_specs=[whole(2, TOK), whole(2, TOK), whole(SLOTS, FEAT + WIDE)],
        out_specs=(whole(UNIT, TOK), whole(TOK, FEAT)),
        out_shape=(struct((UNIT, TOK), BF16), struct((TOK, FEAT), BF16)),
        compiler_params=params("arbitrary"),
        cost_estimate=cost(200_000_000, 1 << 19),
        name="combine",
    )(*far_memory(ids, route), back)
    return hidden_out.T, grad_tokens, grad_mean, grad_rho


def solution(mesh):
    fine = Mesh(mesh.devices.reshape(4, 4, 2, 8), ("x", "y", "core", "expert"))
    dp = ("x", "y", "core")
    in_specs = (
        P("expert", dp),
        P("expert", dp),
        P("expert", None),
        P("expert", None),
        P("expert", None),
        P("expert", dp),
        P("expert", dp, None),
        P("expert", dp, None),
        P("expert", dp, None),
    )
    out_specs = (
        P("expert", dp),
        P("expert", dp),
        P("expert", dp, None),
        P("expert", dp, None),
    )

    return jax.shard_map(
        on_device, mesh=fine, in_specs=in_specs, out_specs=out_specs, check_vma=False
    )
```

```python
import functools

import jax
import jax.numpy as jnp
from jax import lax
from jax.experimental import pallas as pl
from jax.experimental.pallas import tpu as pltpu
from jax.sharding import Mesh, PartitionSpec as P


F32 = jnp.float32
BF16 = jnp.bfloat16
I32 = jnp.int32

EXPERTS = 8
CAP = 40
SLOTS = EXPERTS * CAP
TOK = 128
FEAT = 128
FF = 7168
CHIPS = 16
UNIT = FF // (2 * CHIPS)
WORDS = UNIT // 32
HALF_WORDS = CHIPS * WORDS
WIDE = 256
REST = UNIT - 128
PACK = SLOTS * UNIT // 128
FOLD = PACK - SLOTS
TAIL = SLOTS - FOLD
GROUP = 4 * UNIT
GROUPS = FF // GROUP
PER_STEP = 4
FLAG = 1
DELTA_GROUPS = 2


def iota(shape, dim):
    return lax.broadcasted_iota(I32, shape, dim)


def dot(a, b, dims=((1,), (0,))):
    return lax.dot_general(a, b, (dims, ((), ())), preferred_element_type=F32)


def smem():
    return pl.BlockSpec(memory_space=pltpu.SMEM)


def params(*semantics):
    return pltpu.CompilerParams(
        dimension_semantics=semantics or None, vmem_limit_bytes=16 << 20
    )


def cost(flops, nbytes, trans=0):
    return pl.CostEstimate(flops=flops, bytes_accessed=nbytes, transcendentals=trans)


def ranks_of(ids):
    e = iota((EXPERTS, TOK), 0)
    first = ids[0:1, :] == e
    second = ids[1:2, :] == e
    named = jnp.where(first | second, 1.0, 0.0).astype(BF16)
    before = jnp.where(iota((TOK, TOK), 0) < iota((TOK, TOK), 1), 1.0, 0.0).astype(BF16)
    return first, second, dot(named, before)


def slot_match(mask, rank):
    code = jnp.where(mask, rank, -1.0)
    c = iota((CAP, TOK), 0).astype(F32)
    rows = [
        jnp.where(jnp.broadcast_to(code[e : e + 1, :], (CAP, TOK)) == c, 1.0, 0.0)
        for e in range(EXPERTS)
    ]
    return jnp.concatenate(rows, axis=0)


def sign_bits(words, base):
    lane = iota(words.shape, 1)
    picked = jnp.take_along_axis(
        words, base + lax.shift_right_logical(lane, 5), axis=1, mode="promise_in_bounds"
    )
    return (lax.shift_right_logical(picked, lane & 31) & 1) == 1


def flip(bits, x):
    return jnp.where(bits, -x, x)


def fold(second):
    lane = iota((FOLD, 128), 1)
    tail = second[FOLD:, :]
    moved = [pltpu.roll(tail, (REST - 32 * i) % 128, 1) for i in range(3)]
    return jnp.where(lane < REST, second[:FOLD, :], jnp.concatenate(moved, axis=0))


def unfold(q):
    lane = iota((TAIL, 128), 1)
    r = [pltpu.roll(q[TAIL * i : TAIL * (i + 1), :], 32 * (i + 1), 1) for i in range(3)]
    tail = jnp.where(lane < 32, r[0], jnp.where(lane < 64, r[1], r[2]))
    both = jnp.concatenate([q, tail], axis=0)
    return jnp.where(iota((SLOTS, 128), 1) < REST, both, 0.0)


def place(lin):
    return (lin >> 6) & 3, (lin >> 4) & 3, (lin >> 3) & 1


def chunk_at(lin, k, l):
    x, y, c = place(lin)
    east = (x + jnp.where(c == 0, l, k)) & 3
    north = (y + jnp.where(c == 0, k, l)) & 3
    return 4 * east + north


def step_of(lin, q, other):
    x, y, c = place(lin)
    dx = (x - (q >> 2)) & 3
    dy = (y - (q & 3)) & 3
    swapped = (c == 0) == bool(other)
    return jnp.where(swapped, 4 * dx + dy, 4 * dy + dx)


def hop(array, steps, first):
    pairs = []
    for x in range(4):
        for y in range(4):
            for c in range(2):
                along_y = (c == 0) == first
                to_x, to_y = (x, (y + steps) % 4) if along_y else ((x + steps) % 4, y)
                pairs.append(((x * 4 + y) * 2 + c, (to_x * 4 + to_y) * 2 + c))
    return lax.ppermute(array, ("x", "y", "core"), pairs)


def dispatch_body(core, ids, route, tok, tok_o, ins, ins_o, outs, cot, send_ref):
    c = core[0]
    first, second, rank = ranks_of(ids[...])
    match = slot_match(first | second, rank)
    weight = jnp.where(first, route[0:1, :], jnp.where(second, route[1:2, :], 0.0))
    slot_weight = jnp.concatenate(
        [
            jnp.sum(
                match[CAP * e : CAP * (e + 1), :] * weight[e : e + 1, :], axis=1, keepdims=True
            )
            for e in range(EXPERTS)
        ],
        axis=0,
    )
    hot = match.astype(BF16)
    both = jnp.concatenate([tok[...], tok_o[...]], axis=1)
    send_ref[:, :WIDE] = dot(hot, both).astype(BF16)
    i = iota((HALF_WORDS, FF // 32), 0)
    seventh = lax.shift_right_logical(i * 9363, 16)
    source = 2 * WORDS * seventh + WORDS * c + (i - WORDS * seventh)
    half = jnp.where(iota((HALF_WORDS, FF // 32), 1) == source, 1.0, 0.0).astype(BF16)
    small = jnp.concatenate([ins[...], ins_o[...], jnp.zeros((8, TOK), I32)], axis=0)

    def plane(words, k):
        return (lax.shift_right_logical(words, 8 * k) & 255).astype(F32)

    lows = jnp.concatenate([plane(outs[...], k).astype(BF16) for k in range(4)], axis=1)
    kept = dot(half, lows)
    pieces = [cot[...], jnp.zeros((WIDE - UNIT, TOK), BF16)]
    for k in range(4):
        pieces.append(kept[:, TOK * k : TOK * (k + 1)].astype(BF16))
        pieces.append(plane(small, k).astype(BF16))
    got = dot(hot, jnp.concatenate(pieces, axis=0), ((1,), (1,)))
    send_ref[:, WIDE : 2 * WIDE] = (got[:, :WIDE] * slot_weight).astype(BF16)
    send_ref[:, 2 * WIDE :] = got[:, WIDE:].astype(BF16)


def delta_body(core, mean, rho, noise, own_ref, oth_ref):
    c = core[0]
    lane = iota((FEAT, WIDE), 1)
    for g in range(DELTA_GROUPS):
        lanes = slice(GROUP * g, GROUP * (g + 1))
        u = jnp.exp(rho[0, :, lanes].astype(F32))
        delta = jnp.log(1.0 + u) * noise[0, :, lanes].astype(F32)
        for which, x in ((0, mean[0, :, lanes].astype(F32)), (1, delta)):
            for j in range(4):
                start = UNIT * j
                base = start // 128 * 128
                off = start - base
                width = min(GROUP - base, 384)
                window = x[:, base : base + width]
                if off:
                    window = pltpu.roll(window, width - off, 1)
                chunk = jnp.where(lane < UNIT, window[:, :WIDE], 0.0).astype(BF16)
                at = 2 * g + j // 2

                @pl.when(c == j % 2)
                def _():
                    own_ref[which, at] = chunk

                @pl.when(c != j % 2)
                def _():
                    oth_ref[which, at] = chunk


def forward_part(k, lin, rows, signed, words, weights, halves):
    for l in range(4):
        mean, delta = (
            jnp.concatenate([weights[l][w, 0], weights[4 + l][w, 0]], axis=0) for w in range(2)
        )
        m = dot(rows, mean)
        p = dot(signed, delta)
        base = WORDS * chunk_at(lin, k, l)
        y1 = m[:, :128] + flip(sign_bits(words, base), p[:, :128])
        y2 = m[:, 128:] + flip(sign_bits(words, base + 4), p[:, 128:])
        halves[l // 2][l % 2, :SLOTS, :] = y1.astype(BF16)
        halves[l // 2][l % 2, SLOTS:, :] = fold(y2).astype(BF16)


def forward_first(k, lin, got, *refs):
    weights, halves, (words_ref, signed_ref) = refs[:8], refs[8:10], refs[10:]
    words = jnp.zeros((SLOTS, 128), I32)
    for j in range(4):
        at = 2 * WIDE + 128 * j
        plane = got[:, at : at + 128].astype(F32).astype(I32)
        words = words | lax.shift_left(plane, 8 * j)
    words_ref[...] = words
    for side in range(2):
        bits = sign_bits(words, HALF_WORDS + 4 * side)
        a = got[:, FEAT * side : FEAT * (side + 1)].astype(F32)
        signed_ref[:, FEAT * side : FEAT * (side + 1)] = flip(bits, a).astype(BF16)
    forward_part(k, lin[0], got[:, :WIDE], signed_ref[...], words_ref[...], weights, halves)


def forward_next(k, lin, rows, signed, words, *refs):
    forward_part(k, lin[0], rows[...], signed[...], words[...], refs[:8], refs[8:10])


def join_body(a, b, out_ref):
    out_ref[...] = (a[...].astype(F32) + b[...].astype(F32)).astype(BF16)


def halfway_body(low, low1, low3, high, high1, high3, q0, q1, q2, q3):
    for l, q in enumerate((q0, q1, q2, q3)):
        a, b, c = ((low, low1, low3), (high, high1, high3))[l // 2]
        i = l % 2
        total = a[i].astype(F32) + b[i].astype(F32) + c[i].astype(F32)
        q[...] = total.astype(q.dtype)


def middle_body(q0, t1, t2, t3, up, h_ref, dy_ref):
    total = q0[...] + t1[...].astype(F32) + (t2[...].astype(F32) + t3[...].astype(F32))
    ys = (total[:SLOTS, :], unfold(total[SLOTS:, :]))
    ds = []
    for side, y in enumerate(ys):
        gate = jax.nn.sigmoid(y)
        h_ref[:, 128 * side : 128 * (side + 1)] = (y * gate).astype(BF16)
        u = up[:, 128 * side : 128 * (side + 1)].astype(F32)
        ds.append(u * (gate * (1.0 + y * (1.0 - gate))))
    dy_ref[:SLOTS, :] = ds[0].astype(BF16)
    dy_ref[SLOTS:, :] = fold(ds[1]).astype(BF16)


def stack_body(a, b, c, d, _, low_ref, high_ref):
    for i, x in enumerate((a, b, c, d)):
        (low_ref, high_ref)[i // 2][i % 2] = x[...]


def gradient_chunk(words, dy, k):
    packed = dy.astype(F32)
    d1 = packed[:SLOTS, :]
    d2 = unfold(packed[SLOTS:, :])
    plain = jnp.concatenate([d1, d2], axis=1).astype(BF16)
    signed = jnp.concatenate(
        [
            flip(sign_bits(words, WORDS * k), d1),
            flip(sign_bits(words, WORDS * k + 4), d2),
        ],
        axis=1,
    ).astype(BF16)
    return plain, signed


def weight_gradients(l, rows_t, signed_t, plain, signed, mine_ref, theirs_ref):
    for which, g in ((0, dot(rows_t, plain)), (1, dot(signed_t, signed))):
        mine_ref[which, l] = g[:FEAT, :].astype(BF16)
        theirs_ref[which, l] = g[FEAT:, :].astype(BF16)


def gradient_part(k, lin, words, dys, weights, sums, turned=None, outs=None):
    plains = []
    signeds = []
    for l in range(4):
        dy = dys[l // 2][l % 2]
        plain, signed = gradient_chunk(words, dy, chunk_at(lin, -k, -l))
        plains.append(plain)
        signeds.append(signed)
        if outs is not None:
            weight_gradients(l, *turned, plain, signed, *outs)
    out = []
    for which, parts in ((0, plains), (1, signeds)):
        side = [
            jnp.concatenate([w[which, 0] for w in weights[at : at + 4]], axis=1) for at in (0, 4)
        ]
        total = dot(
            jnp.concatenate(parts, axis=1), jnp.concatenate(side, axis=0), ((1,), (1,))
        )
        out.append(total if sums is None else total + sums[which][...])
    return out


def gradient_first(lin, words, rows, low, high, *refs):
    dys = (low, high)
    weights, (mine, theirs, rows_t, signed_t, sum_m, sum_d) = refs[:8], refs[8:]
    for side in range(2):
        lanes = slice(FEAT * side, FEAT * (side + 1))
        a = rows[:, lanes].astype(F32)
        bits = sign_bits(words[...], HALF_WORDS + 4 * side)
        rows_t[lanes, :] = a.T.astype(BF16)
        signed_t[lanes, :] = flip(bits, a).T.astype(BF16)
    sum_m[...], sum_d[...] = gradient_part(
        0, lin[0], words[...], dys, weights, None, (rows_t[...], signed_t[...]), (mine, theirs)
    )


def gradient_next(k, lin, words, rows_t, signed_t, in_m, in_d, low, high, *refs):
    weights, (_, _, mine, theirs, sum_m, sum_d) = refs[:8], refs[8:]
    sum_m[...], sum_d[...] = gradient_part(
        k, lin[0], words[...], (low, high), weights, (in_m, in_d),
        (rows_t[...], signed_t[...]), (mine, theirs),
    )


def gradient_last(k, lin, words, in_m, in_d, low, high, *refs):
    weights, (g_ref, g_away_ref) = refs[:8], refs[8:]
    total_m, total_d = gradient_part(
        k, lin[0], words[...], (low, high), weights, (in_m, in_d)
    )
    for side, ref in ((0, g_ref), (1, g_away_ref)):
        lanes = slice(FEAT * side, FEAT * (side + 1))
        bits = sign_bits(words[...], HALF_WORDS + 4 * side)
        ref[...] = total_m[:, lanes] + flip(bits, total_d[:, lanes])


def late_body(lin, words, rows_t, signed_t, low, high, _, mine_ref, theirs_ref):
    for l in range(4):
        plain, signed = gradient_chunk(
            words[...], (low, high)[l // 2][l % 2], chunk_at(lin[0], -2, -l)
        )
        weight_gradients(
            l, rows_t[...], signed_t[...], plain, signed, mine_ref, theirs_ref
        )


def slots_body(g, g_near, hidden, send_ref):
    send_ref[:, :FEAT] = (g[...] + g_near[...]).astype(BF16)
    send_ref[:, FEAT:] = hidden[...]


def assemble_body(lin, *refs):
    _, _, c = place(lin[0])
    mine, early, late = refs[:4], refs[4:8], refs[8:12]
    rho, noise, gm_ref, gr_ref = refs[12:]
    step = pl.program_id(0)

    def laid(which, at):
        out = []
        for i in (at, at + 1):
            came_early = step_of(lin[0], PER_STEP * step + i, 1) >> 2 != 2
            theirs = jnp.where(came_early, early[i][which, 0], late[i][which, 0])
            for p in range(2):
                out.append(jnp.where(c == p, mine[i][which, 0], theirs)[:, :UNIT])
        return jnp.concatenate([x.astype(F32) for x in out], axis=1)

    for half in range(PER_STEP // 2):
        lanes = slice(GROUP * half, GROUP * (half + 1))
        gm_ref[0, :, lanes] = laid(0, 2 * half).astype(BF16)
        e = jnp.exp(rho[0, :, lanes].astype(F32))
        factor = noise[0, :, lanes].astype(F32) * (e / (1.0 + e))
        gr_ref[0, :, lanes] = (laid(1, 2 * half) * factor).astype(BF16)


def combine_body(ids, route, got, hidden_ref, tokens_ref):
    first, second, rank = ranks_of(ids[...])
    total = jnp.zeros((WIDE, TOK), F32)
    both = jnp.zeros((SLOTS, TOK), F32)
    for k, mask in enumerate((first, second)):
        match = slot_match(mask, rank)
        both = both + match
        picked = dot(got[:, FEAT:], match.astype(BF16), ((0,), (0,)))
        total = total + picked * route[k : k + 1, :]
    hidden_ref[...] = total[:UNIT, :].astype(BF16)
    tokens_ref[...] = dot(both.astype(BF16), got[:, :FEAT], ((0,), (0,))).astype(BF16)


def whole(*shape):
    return pl.BlockSpec(shape, lambda *_: (0,) * len(shape))


def far_memory(*xs):
    return [pltpu.with_memory_space_constraint(x, pltpu.HBM) for x in xs]


def struct(shape, dtype):
    return jax.ShapeDtypeStruct(shape, dtype)


def on_device(
    tokens, in_signs, out_signs, expert_ids, route_weight, cotangent,
    mean_weight, rho_weight, noise_weight,
):
    mean_weight, rho_weight, noise_weight = far_memory(mean_weight, rho_weight, noise_weight)
    core = lax.axis_index("core").astype(I32).reshape(1)
    lin = lax.axis_index(("x", "y", "core", "expert")).astype(I32).reshape(1)
    swap = [(0, 1), (1, 0)]
    ids = expert_ids.T
    route = route_weight.T
    ins = in_signs.T

    tok_o = lax.ppermute(tokens, "core", swap)
    ins_o = lax.ppermute(ins, "core", swap)

    raw = far_memory(ids, route, tokens)
    raw += [tok_o, *far_memory(ins), ins_o, *far_memory(out_signs.T, cotangent.T)]
    send = pl.pallas_call(
        dispatch_body,
        grid=(1,),
        in_specs=[smem()] + [whole(*x.shape) for x in raw],
        out_specs=whole(SLOTS, 4 * WIDE),
        out_shape=struct((SLOTS, 4 * WIDE), BF16),
        compiler_params=params("arbitrary"),
        cost_estimate=cost(400_000_000, 1 << 20),
        name="dispatch",
    )(core, *raw)

    def exchange(x):
        wide = x.reshape(EXPERTS, CAP, x.shape[1])
        got = lax.all_to_all(wide, "expert", split_axis=0, concat_axis=0, tiled=True)
        return got.reshape(x.shape)

    got = exchange(send)

    late, _ = lax.optimization_barrier((core, send))
    block = pl.BlockSpec((1, FEAT, DELTA_GROUPS * GROUP), lambda g: (0, 0, g))
    pair = pl.BlockSpec((2, 2 * DELTA_GROUPS, FEAT, WIDE), lambda g: (0, g, 0, 0))
    own, away = pl.pallas_call(
        delta_body,
        grid=(GROUPS // DELTA_GROUPS,),
        in_specs=[smem(), block, block, block],
        out_specs=(pair, pair),
        out_shape=(pltpu.HBM((2, CHIPS, FEAT, WIDE), BF16),) * 2,
        compiler_params=params("arbitrary"),
        cost_estimate=cost(2_000_000_000, 10 << 20, 2 * FEAT * FF),
        name="delta",
    )(late, mean_weight, rho_weight, noise_weight)
    near = lax.ppermute(away, "core", swap)

    steps = CHIPS // PER_STEP
    table = whole(SLOTS, 128)
    rows_spec = pl.BlockSpec((SLOTS, WIDE), lambda *_: (0, 0))
    half = struct((2, PACK, 128), BF16)
    half_spec = whole(2, PACK, 128)
    lone_spec = whole(PACK, 128)

    def picked(index):
        return pl.BlockSpec(
            (2, 1, FEAT, WIDE), lambda i, lin: (0, index(lin[0], i), 0, 0)
        )

    def grid_spec(n, ins, outs, scratch=()):
        return pltpu.PrefetchScalarGridSpec(
            num_scalar_prefetch=1, grid=(n,), in_specs=ins, out_specs=outs,
            scratch_shapes=scratch,
        )

    (own_far,) = far_memory(own)
    sent = [[] for _ in range(4)]
    words = signed = None
    for k in (2, 1, 3, 0):
        chunks = [
            picked(lambda lin, i, k=k, l=l: chunk_at(lin, k, l)) for l in range(4)
        ] * 2
        if words is None:
            *sent[k], words, signed = pl.pallas_call(
                functools.partial(forward_first, k),
                grid_spec=grid_spec(
                    1, [whole(SLOTS, 4 * WIDE), *chunks], (half_spec, half_spec, table, rows_spec)
                ),
                out_shape=(
                    half, half, struct((SLOTS, 128), I32), struct((SLOTS, WIDE), BF16)
                ),
                compiler_params=params("arbitrary"),
                cost_estimate=cost(600_000_000, 2 << 20),
            )(lin, got, *[own_far] * 4, *[near] * 4)
        else:
            sent[k] = pl.pallas_call(
                functools.partial(forward_next, k),
                grid_spec=grid_spec(
                    1, [rows_spec, rows_spec, table, *chunks], (half_spec, half_spec)
                ),
                out_shape=(half, half),
                compiler_params=params("arbitrary"),
                cost_estimate=cost(600_000_000, 2 << 20),
            )(lin, got, signed, words, *[own] * 4, *[near] * 4)

    def move(x, steps):
        return hop(x, steps, True)

    def joined(x, y):
        return pl.pallas_call(
            join_body,
            grid=(1,),
            in_specs=[half_spec, half_spec],
            out_specs=half_spec,
            out_shape=half,
            compiler_params=params("arbitrary"),
            cost_estimate=cost(50_000_000, 1 << 20),
        )(x, y)

    from_below = move(sent[2][0], 1)
    from_above = move(sent[2][1], 3)
    high1 = move(sent[1][1], 1)
    low3 = move(sent[3][0], 3)
    low1 = move(joined(sent[1][0], from_below), 1)
    high3 = move(joined(sent[3][1], from_above), 3)
    lone = struct((PACK, 128), BF16)
    kept, *passed = pl.pallas_call(
        halfway_body,
        grid=(1,),
        in_specs=[half_spec] * 6,
        out_specs=(lone_spec,) * 4,
        out_shape=(struct((PACK, 128), F32), lone, lone, lone),
        compiler_params=params("arbitrary"),
        cost_estimate=cost(200_000_000, 3 << 20),
        name="halfway",
    )(sent[0][0], low1, low3, sent[0][1], high1, high3)
    passed = [hop(passed[l - 1], l, False) for l in (1, 2, 3)]
    hidden, dy = pl.pallas_call(
        middle_body,
        grid=(1,),
        in_specs=[lone_spec] * 4 + [pl.BlockSpec((SLOTS, WIDE), lambda *_: (0, 1))],
        out_specs=(whole(SLOTS, WIDE), lone_spec),
        out_shape=(struct((SLOTS, WIDE), BF16), lone),
        compiler_params=params("arbitrary"),
        cost_estimate=cost(200_000_000, 1 << 20),
        name="middle",
    )(kept, *passed, got)
    beside = [hop(dy, l, False) for l in (1, 2, 3)]
    partner = lax.ppermute(beside[FLAG], "core", swap)
    low, high = pl.pallas_call(
        stack_body,
        grid=(1,),
        in_specs=[lone_spec] * 4 + [pl.BlockSpec(memory_space=pl.ANY)],
        out_specs=(half_spec, half_spec),
        out_shape=(half, half),
        compiler_params=params("arbitrary"),
        cost_estimate=cost(100_000_000, 1 << 20),
        name="stack",
    )(dy, *beside, partner)
    low1 = move(low, 1)
    high3 = move(high, 3)
    high1 = move(high, 1)
    low3 = move(low, 3)
    low2 = move(low1, 1)
    high2 = move(high3, 3)
    dys = [(low, high), (low1, high1), (low2, high2), (low3, high3)]

    sums = whole(SLOTS, FEAT)
    wide_sums = whole(SLOTS, WIDE)
    turned = whole(WIDE, SLOTS)
    side = pltpu.HBM((2, CHIPS, FEAT, WIDE), BF16)
    in_place = pl.BlockSpec(memory_space=pltpu.HBM)
    turned_shape = struct((WIDE, SLOTS), BF16)
    total_shape = struct((SLOTS, WIDE), F32)
    slot_shape = struct((SLOTS, FEAT), F32)
    part = pltpu.HBM((2, 12, FEAT, WIDE), BF16)
    rest_part = pltpu.HBM((2, 4, FEAT, WIDE), BF16)
    for k in (0, 1, 3, 2):
        chunks = [
            picked(lambda lin, i, k=k, l=l: chunk_at(lin, -k, -l)) for l in range(4)
        ] * 2
        block = pl.BlockSpec((2, 4, FEAT, WIDE), lambda i, lin, k=k: (0, k, 0, 0))
        carried = (mine, theirs) if k in (1, 3) else ()
        away_block = pl.BlockSpec(
            (2, 4, FEAT, WIDE), lambda i, lin, k=k: (0, min(k, 2), 0, 0)
        )
        if k == 0:
            body = gradient_first
            ins = [table, rows_spec, half_spec, half_spec, *chunks]
            outs = (block, away_block, turned, turned, wide_sums, wide_sums)
            shapes = (side, part, turned_shape, turned_shape, total_shape, total_shape)
            operands = (words, got, *dys[k])
        elif k != 2:
            body = functools.partial(gradient_next, k)
            ins = [table, turned, turned, wide_sums, wide_sums, half_spec, half_spec, *chunks]
            ins += [in_place, in_place]
            outs = (block, away_block, wide_sums, wide_sums)
            shapes = (side, part, total_shape, total_shape)
            operands = (words, rows_t, signed_t, *totals, *dys[k])
        else:
            body = functools.partial(gradient_last, k)
            ins = [table, wide_sums, wide_sums, half_spec, half_spec, *chunks]
            outs = (sums, sums)
            shapes = (slot_shape,) * 2
            operands = (words, *totals, *dys[k])
        rest = pl.pallas_call(
            body,
            grid_spec=grid_spec(1, ins, outs),
            out_shape=shapes,
            input_output_aliases={len(ins) - 1: 0, len(ins): 1} if carried else {},
            compiler_params=params("arbitrary"),
            cost_estimate=cost(1_300_000_000, 3 << 20),
        )(lin, *operands, *[own] * 4, *[near] * 4, *carried)
        if k != 2:
            mine, theirs, *rest = rest
        if k == 0:
            rows_t, signed_t, *rest = rest
        totals = rest
    g, g_away = totals
    g_near = lax.ppermute(g_away, "core", swap)
    theirs, _ = lax.optimization_barrier((theirs, g_near))
    theirs = lax.ppermute(theirs, "core", swap)
    send = pl.pallas_call(
        slots_body,
        grid=(1,),
        in_specs=[sums, sums, whole(SLOTS, WIDE)],
        out_specs=whole(SLOTS, FEAT + WIDE),
        out_shape=struct((SLOTS, FEAT + WIDE), BF16),
        compiler_params=params("arbitrary"),
        cost_estimate=cost(100_000_000, 1 << 20),
        name="slots",
    )(g, g_near, hidden)
    back = exchange(send)
    late, _ = lax.optimization_barrier((lin, send))
    mine, tail = pl.pallas_call(
        late_body,
        grid_spec=grid_spec(
            1,
            [table, turned, turned, half_spec, half_spec, in_place],
            (
                pl.BlockSpec((2, 4, FEAT, WIDE), lambda i, lin: (0, 2, 0, 0)),
                whole(2, 4, FEAT, WIDE),
            ),
        ),
        out_shape=(side, rest_part),
        input_output_aliases={6: 0},
        compiler_params=params("arbitrary"),
        cost_estimate=cost(1_500_000_000, 6 << 20),
        name="late",
    )(late, *far_memory(words, rows_t, signed_t, *dys[2]), mine)
    tail = lax.ppermute(tail, "core", swap)
    wide = pl.BlockSpec((1, FEAT, FF // steps), lambda g, lin: (0, 0, g))

    def early_place(slot):
        return jnp.where(slot < 8, slot, 8 + (slot & 3))

    def late_place(slot):
        return slot & 3

    laid = [
        picked(lambda lin, i, l=l, f=f, other=other: f(step_of(lin, 4 * i + l, other)))
        for f, other in ((lambda slot: slot, 0), (early_place, 1), (late_place, 1))
        for l in range(4)
    ]
    grad_mean, grad_rho = pl.pallas_call(
        assemble_body,
        grid_spec=grid_spec(steps, [*laid, wide, wide], (wide, wide)),
        out_shape=(struct((1, FEAT, FF), BF16),) * 2,
        compiler_params=params("arbitrary"),
        cost_estimate=cost(3_000_000_000, 12 << 20, FEAT * FF),
        name="assemble",
    )(late, *far_memory(*[mine] * 4), *[theirs] * 4, *[tail] * 4, rho_weight, noise_weight)

    hidden_out, grad_tokens = pl.pallas_call(
        combine_body,
        grid=(1,),
        in_specs=[whole(2, TOK), whole(2, TOK), whole(SLOTS, FEAT + WIDE)],
        out_specs=(whole(UNIT, TOK), whole(TOK, FEAT)),
        out_shape=(struct((UNIT, TOK), BF16), struct((TOK, FEAT), BF16)),
        compiler_params=params("arbitrary"),
        cost_estimate=cost(200_000_000, 1 << 19),
        name="combine",
    )(ids, route, back)
    return hidden_out.T, grad_tokens, grad_mean, grad_rho


def solution(mesh):
    fine = Mesh(mesh.devices.reshape(4, 4, 2, 8), ("x", "y", "core", "expert"))
    dp = ("x", "y", "core")
    in_specs = (
        P("expert", dp),
        P("expert", dp),
        P("expert", None),
        P("expert", None),
        P("expert", None),
        P("expert", dp),
        P("expert", dp, None),
        P("expert", dp, None),
        P("expert", dp, None),
    )
    out_specs = (
        P("expert", dp),
        P("expert", dp),
        P("expert", dp, None),
        P("expert", dp, None),
    )

    return jax.shard_map(
        on_device, mesh=fine, in_specs=in_specs, out_specs=out_specs, check_vma=False
    )
```
